16 devices in a mesh: batch: 2 (over y, z), g: 8 (over x, core).
Axes of the slice: x: 4, y: 2, z: 1, core: 2. Of those that a mesh axis runs over, the one named last changes fastest.
The devices are a block of a 4x4x8 slice.
Arguments:
- keys: float32 [131072], P(('batch', 'g')), parts along dimension 0
- payload: bfloat16 [131072, 256], P(('batch', 'g')), parts along dimension 0
Outputs:
- output 1: float32 [262144], P(('batch', 'g')), parts along dimension 0
- output 2: bfloat16 [262144, 256], P(('batch', 'g')), parts along dimension 0
- output 3: int32 [16], P(('batch', 'g')), parts along dimension 0
There are 2 independent parts. The reference program is written for one: setup_inputs(seed, part) draws one part's arguments, and reference() takes and returns one part's arrays. A program takes and returns all parts, laid end to end along the dimension named above; each array names one.
All inputs are finite; a program needn't handle non-finite values.
Results may differ from the reference program's by a relative error of at most 0.001.
Values are sent between devices in bfloat16 or wider.
A program may use at most 768 MiB of HBM per device.

```python
import math
import functools
import jax
import jax.numpy as jnp
from jax import lax

GROUP = 8
N_DEV = 8192
WIDTH = 256
SEGMENTS = 16
PART_ROWS = GROUP * N_DEV
OUT_ROWS = 2 * N_DEV
PAD_KEY = 128.0


def swap_into(perm_row, dev_id, target):
    cur_pos = jnp.argmax(perm_row == dev_id)
    displaced = perm_row[target]
    slot_ids = jnp.arange(perm_row.shape[0])
    return jnp.where(slot_ids == target, dev_id, jnp.where(slot_ids == cur_pos, displaced, perm_row))


def draw_keys(base):
    k_gap, k_exp, k_pick, k_block, k_heads, k_rest, k_local = jax.random.split(base, 7)
    seg_exp = jax.random.randint(k_exp, (SEGMENTS, 1), 0, 8)
    raw_bits = jax.random.randint(k_gap, (SEGMENTS, PART_ROWS // SEGMENTS), 0, 128)
    levels = jnp.cumsum((1 + jnp.right_shift(raw_bits, 7 - seg_exp)).reshape(-1))
    centered = levels - levels[PART_ROWS // 2]
    key_scale = 2.0 ** -(int(math.log2(PART_ROWS)) + 2)
    ranked_keys = centered.astype(jnp.float32) * key_scale
    picked = jax.random.permutation(k_pick, GROUP)
    hot_dev = picked[0]
    cold_dev = picked[1]
    hot_block = jax.random.randint(k_block, (), 0, GROUP - 1)
    block_ids = jnp.arange(GROUP)[:, None]
    head_owner = jax.vmap(functools.partial(jax.random.permutation, x=GROUP))(jax.random.split(k_heads, GROUP))
    hot_row = head_owner[hot_block]
    hot_pos = jnp.argmax(hot_row == hot_dev)
    hot_row = swap_into(hot_row, hot_dev, jnp.where(hot_pos >= GROUP // 2, hot_pos, GROUP - 1))
    head_owner = jnp.where(block_ids == hot_block, hot_row[None, :], head_owner)
    next_row = swap_into(head_owner[hot_block + 1], hot_dev, 0)
    head_owner = jnp.where(block_ids == hot_block + 1, next_row[None, :], head_owner)
    tail_owner = jnp.broadcast_to(jnp.repeat(jnp.arange(GROUP), N_DEV // GROUP - 1)[None, :], (GROUP, N_DEV - GROUP))
    tail_owner = jnp.where((block_ids == hot_block) & (tail_owner == cold_dev), hot_dev, tail_owner)
    tail_owner = jnp.where((block_ids == hot_block + 1) & (tail_owner == hot_dev), cold_dev, tail_owner)
    tail_owner = jax.vmap(jax.random.permutation)(jax.random.split(k_rest, GROUP), tail_owner)
    owners = jnp.concatenate([head_owner, tail_owner], axis=1).reshape(-1)
    rank_grid = jnp.argsort(owners, stable=True).reshape(GROUP, N_DEV)
    rank_grid = jax.vmap(jax.random.permutation)(jax.random.split(k_local, GROUP), rank_grid)
    return ranked_keys[rank_grid.reshape(-1)]


def setup_inputs(seed: int = 0, part: int = 0) -> dict:
    base = jax.random.fold_in(jax.random.key(seed), part)
    k_keys, k_rows = jax.random.split(base)
    keys = draw_keys(k_keys)
    payload = jax.random.normal(k_rows, (PART_ROWS, WIDTH), jnp.float32).astype(jnp.bfloat16)
    return {"keys": keys, "payload": payload}


def reference(keys, payload):
    local_sorted = jnp.sort(keys.reshape(GROUP, N_DEV), axis=1)
    samples = local_sorted[:, :: N_DEV // GROUP].reshape(-1)
    splitters = jnp.sort(samples)[GROUP + GROUP // 2 :: GROUP]
    sorted_all, sort_order = lax.sort((keys, jnp.arange(PART_ROWS, dtype=jnp.int32)), num_keys=1)
    edges = jnp.searchsorted(sorted_all, splitters, side="left").astype(jnp.int32)
    starts = jnp.concatenate([jnp.zeros((1,), jnp.int32), edges])
    stops = jnp.concatenate([edges, jnp.full((1,), PART_ROWS, jnp.int32)])
    counts = stops - starts
    slot_ids = jnp.arange(OUT_ROWS, dtype=jnp.int32)
    src_pos = jnp.minimum(starts[:, None] + slot_ids[None, :], PART_ROWS - 1)
    is_valid = slot_ids[None, :] < counts[:, None]
    out_keys = jnp.where(is_valid, sorted_all[src_pos], PAD_KEY)
    out_payload = jnp.where(is_valid[:, :, None], payload[sort_order[src_pos]], 0.0)
    return out_keys.reshape(-1), out_payload.reshape(-1, WIDTH), counts
```

```python
import jax
import jax.numpy as jnp
from jax import lax
from jax.sharding import PartitionSpec as P

PAD_KEY = 128.0


def solution(mesh):
    group = mesh.shape["g"]

    def local_part(keys_loc, rows_loc):
        n = keys_loc.shape[0]
        width = rows_loc.shape[1]
        cap = 2 * n // group
        me = lax.axis_index("g")
        sorted_keys, order = lax.sort((keys_loc, lax.iota(jnp.int32, n)), num_keys=1)
        all_keys = lax.all_gather(sorted_keys, "g")
        samples = all_keys[:, :: n // group].reshape(-1)
        ranks = jnp.sum(samples[None, :] < samples[:, None], axis=1)
        want = group + group // 2 + group * lax.iota(jnp.int32, group - 1)
        splitters = jnp.sum(jnp.where(ranks[None, :] == want[:, None], samples[None, :], 0.0), axis=1)
        edges = jnp.sum(all_keys[:, None, :] < splitters[None, :, None], axis=-1).astype(jnp.int32)
        starts = jnp.concatenate([jnp.zeros((group, 1), jnp.int32), edges], axis=1)
        stops = jnp.concatenate([edges, jnp.full((group, 1), n, jnp.int32)], axis=1)
        counts = stops - starts
        slot = lax.iota(jnp.int32, cap)
        order_pad = jnp.concatenate([order, jnp.zeros((cap,), jnp.int32)])
        my_starts = lax.dynamic_index_in_dim(starts, me, 0, keepdims=False)
        send_idx = jnp.concatenate([lax.dynamic_slice(order_pad, (my_starts[d],), (cap,)) for d in range(group)])
        send_rows = rows_loc[send_idx].reshape(group, cap, width)
        recv_rows = lax.all_to_all(send_rows, "g", 0, 0, tiled=True)
        in_starts = lax.dynamic_index_in_dim(starts, me, 1, keepdims=False)
        in_counts = lax.dynamic_index_in_dim(counts, me, 1, keepdims=False)
        key_pad = jnp.concatenate([all_keys, jnp.full((group, cap), PAD_KEY)], axis=1)
        wins = []
        for s in range(group):
            win = lax.dynamic_slice(key_pad[s], (in_starts[s],), (cap,))
            wins.append(jnp.where(slot < in_counts[s], win, PAD_KEY))
        merged_keys, merge_order = lax.sort((jnp.concatenate(wins), lax.iota(jnp.int32, 2 * n)), num_keys=1)
        own = jnp.sum(in_counts)
        merged_rows = recv_rows.reshape(-1, width)[merge_order]
        merged_rows = jnp.where((lax.iota(jnp.int32, 2 * n) < own)[:, None], merged_rows, 0.0)
        return merged_keys, merged_rows, own.reshape(1)

    row_spec = P(("batch", "g"))
    mat_spec = P(("batch", "g"), None)
    return jax.shard_map(local_part, mesh=mesh, in_specs=(row_spec, mat_spec), out_specs=(row_spec, mat_spec, row_spec), check_vma=False)
```

```python
import functools

import jax
import jax.numpy as jnp
from jax import lax
from jax.experimental import pallas as pl
from jax.experimental.pallas import tpu as pltpu
from jax.sharding import PartitionSpec as P

PAD_KEY = 128.0
LANES = 128
MESH = pl.DeviceIdType.MESH


def greet(group):
    me = lax.axis_index("g")
    barrier = pltpu.get_barrier_semaphore()
    for off in range(1, group):
        pl.semaphore_signal(barrier, inc=1, device_id={"g": lax.rem(me + off, group)}, device_id_type=MESH)
    pl.semaphore_wait(barrier, group - 1)
    return me


def lane_prefix(x, lane):
    for step in (1, 2, 4):
        x = x + jnp.where(lane >= step, pltpu.roll(x, step, 1), 0)
    return x


def sub_prefix(x, sub):
    for step in (1, 2, 4):
        x = x + jnp.where(sub >= step, pltpu.roll(x, step, 0), 0)
    return x


def plan_kernel(group, n, cap, relay, keys_ref, rows_ref,
                win_ref, loc_ref, rows3_ref, tab_ref, idx1_ref, idx2_ref, info_ref,
                all_keys, tab_smem, send_sem, recv_sem, tab_sem):
    run_rows = n // LANES
    win_rows = 2 * run_rows // group
    me = greet(group)
    copies = []
    for off in range(1, group):
        copy = pltpu.make_async_remote_copy(
            src_ref=keys_ref, dst_ref=all_keys.at[me, pl.ds(0, run_rows)], send_sem=send_sem.at[off],
            recv_sem=recv_sem.at[off], device_id={"g": lax.rem(me + off, group)}, device_id_type=MESH)
        copy.start()
        copies.append(copy)
    all_keys[me, pl.ds(0, run_rows)] = keys_ref[...]
    tail = all_keys.shape[1] - run_rows
    for s in range(group):
        all_keys[s, pl.ds(run_rows, tail)] = jnp.full((tail, LANES), PAD_KEY, jnp.float32)

    def relayout(t, c):
        at = pl.multiple_of(t * 64, 64)
        rows3_ref[pl.ds(at, 64)] = rows_ref[pl.ds(at, 64)].reshape(64, 2, LANES)
        return c

    lax.fori_loop(0, n // 64, relayout, 0)
    for copy in copies:
        copy.wait()

    count = group * group
    stride = run_rows // group
    col = jnp.concatenate(
        [jnp.concatenate([all_keys[s, pl.ds(m * stride, 1)] for m in range(group)], axis=0) for s in range(group)], axis=0)
    col = jnp.broadcast_to(col[:, 0:1], (count, LANES))
    r_id = lax.broadcasted_iota(jnp.int32, (count, LANES), 0)
    l_id = lax.broadcasted_iota(jnp.int32, (count, LANES), 1)
    row = jnp.sum(jnp.where(r_id == l_id, col, 0.0), axis=0, keepdims=True)
    less = (jnp.broadcast_to(row, (count, LANES)) < col) & (l_id < count)
    rank = jnp.sum(jnp.where(less, 1.0, 0.0), axis=1, keepdims=True)
    want = (group * l_id + group // 2).astype(jnp.float32)
    splitters = jnp.sum(jnp.where(jnp.broadcast_to(rank, (count, LANES)) == want, col, 0.0), axis=0, keepdims=True)

    lane = lax.broadcasted_iota(jnp.int32, (group, LANES), 1)
    sub = lax.broadcasted_iota(jnp.int32, (group, LANES), 0)
    edges = jnp.where(lane < group, 0, n)
    for j in range(1, group):
        part = []
        for s in range(group):
            hit = jnp.where(all_keys[s, pl.ds(0, run_rows)] < splitters[0, j], 1, 0)
            part.append(jnp.sum(hit, axis=0, keepdims=True))
        total = jnp.sum(jnp.concatenate(part, axis=0), axis=1, keepdims=True)
        edges = jnp.where(lane == j, jnp.broadcast_to(total, (group, LANES)), edges)
    counts = jnp.where(lane < group, pltpu.roll(edges, LANES - 1, 1) - edges, 0)
    over = jnp.maximum(counts - cap, 0)
    share = jnp.right_shift(over + (group - 1), group.bit_length() - 1)
    first = lane_prefix(share, lane) - share
    second = sub_prefix(share, sub) - share
    worst = jnp.maximum(jnp.max(first + share), jnp.max(second + share))
    tab_ref[0] = edges
    tab_ref[1] = counts
    tab_ref[2] = share
    tab_ref[3] = first
    tab_ref[4] = second
    to_smem = pltpu.make_async_copy(tab_ref, tab_smem, tab_sem)
    to_smem.start()
    to_smem.wait()

    idx1 = jnp.zeros((group, LANES), jnp.int32)
    for j in range(group):
        q, a = tab_smem[2, me, j], tab_smem[3, me, j]
        src = tab_smem[0, me, j] + cap - a + q * sub + lane
        idx1 = jnp.where((lane >= a) & (lane < a + q), src, idx1)
    idx1_ref[...] = jnp.clip(idx1, 0, n - 1)
    lane1 = lane[0:1]
    for j in range(group):
        line = jnp.zeros((1, LANES), jnp.int32)
        for s in range(group):
            q, a, b = tab_smem[2, s, j], tab_smem[3, s, j], tab_smem[4, s, j]
            line = jnp.where((lane1 >= b) & (lane1 < b + q), s * relay + a - b + lane1, line)
        idx2_ref[pl.ds(j, 1)] = jnp.clip(line, 0, group * relay - 1)

    wl = lax.broadcasted_iota(jnp.int32, (win_rows, LANES), 1)
    pos = lax.broadcasted_iota(jnp.int32, (win_rows, LANES), 0) * LANES + wl
    own = jnp.int32(0)
    for s in range(group):
        start, num = tab_smem[0, s, me], tab_smem[1, s, me]
        q, b = tab_smem[2, s, me], tab_smem[4, s, me]
        own = own + num
        shift = jnp.bitwise_and(start, LANES - 1)
        at = jnp.right_shift(start, LANES.bit_length() - 1)
        turn = jnp.bitwise_and(LANES - shift, LANES - 1)
        one = pltpu.roll(all_keys[s, pl.ds(at, win_rows)], turn, 1)
        two = pltpu.roll(all_keys[s, pl.ds(at + 1, win_rows)], turn, 1)
        window = jnp.where(wl < LANES - shift, one, two)
        win_ref[pl.ds(s * win_rows, win_rows)] = jnp.where(pos < num, window, PAD_KEY)
        extra = pos - cap
        far = group * cap + b + extra
        for m in range(1, group):
            far = far + jnp.where(extra >= m * q, relay - q, 0)
        loc = jnp.where(pos < cap, s * cap + pos, far)
        loc_ref[pl.ds(s * win_rows, win_rows)] = jnp.where(pos < num, jnp.clip(loc, 0, group * (cap + relay) - 1), 0)
    info_ref[0] = own
    info_ref[1] = jnp.where(worst <= relay, 1, 0)


def exchange_kernel(group, cap, relay, unroll, order_ref, start_ref, idx1_ref, idx2_ref, rows_ref,
                    out_ref, near, far1, far2, got, near_sems, far1_sems, far2_sems):
    me = greet(group)

    def gather(dst, base, size, pick):
        def step(t, c):
            for u in range(unroll):
                r = t * unroll + u
                dst[base + r] = pick(r)
            return c
        lax.fori_loop(0, size // unroll, step, 0)

    def send(src, dst, sems, off):
        copy = pltpu.make_async_remote_copy(
            src_ref=src, dst_ref=dst, send_sem=sems.at[0, off], recv_sem=sems.at[1, off],
            device_id={"g": lax.rem(me + off, group)}, device_id_type=MESH)
        copy.start()
        return copy

    offsets = [2, 6, 4, 3, 7, 5, 1]
    firsts, others = [], []
    for off in offsets + [0]:
        peer = lax.rem(me + off, group)
        pick = lambda r: rows_ref[order_ref[idx1_ref[peer, r]]]
        if off:
            gather(far1.at[off], 0, relay, pick)
            firsts.append(send(far1.at[off], got.at[pl.ds(me * relay, relay)], far1_sems, off))
        else:
            gather(got, me * relay, relay, pick)
    for off in offsets + [0]:
        start = start_ref[lax.rem(me + off, group)]
        pick = lambda r: rows_ref[order_ref[start + r]]
        if off:
            gather(near.at[off], 0, cap, pick)
            others.append(send(near.at[off], out_ref.at[pl.ds(me * cap, cap)], near_sems, off))
        else:
            gather(out_ref, me * cap, cap, pick)
    for copy in firsts:
        copy.wait()
    base2 = group * cap + me * relay
    for off in offsets + [0]:
        peer = lax.rem(me + off, group)
        pick = lambda r: got[idx2_ref[peer, r]]
        if off:
            gather(far2.at[off], 0, relay, pick)
            others.append(send(far2.at[off], out_ref.at[pl.ds(base2, relay)], far2_sems, off))
        else:
            gather(out_ref, base2, relay, pick)
    for copy in others:
        copy.wait()


def place_kernel(block, unroll, loc_ref, info_ref, rows_ref, out_ref, tmp):
    base = pl.program_id(0) * block
    num = jnp.clip(info_ref[0] - base, 0, block)
    width = out_ref.shape[1]

    def step(t, c):
        for u in range(unroll):
            r = t * unroll + u
            tmp[r] = rows_ref[loc_ref[base + r]]
        return c

    lax.fori_loop(0, (num + unroll - 1) // unroll, step, 0)

    def finish(t, c):
        at = pl.multiple_of(t * 64, 64)
        x = tmp[pl.ds(at, 64)].reshape(64, width)
        row = at + lax.broadcasted_iota(jnp.int32, (64, width), 0)
        out_ref[pl.ds(at, 64)] = jnp.where(row < num, x, jnp.zeros_like(x))
        return c

    full = (num + 63) // 64
    lax.fori_loop(0, full, finish, 0)

    def blank(t, c):
        at = pl.multiple_of(t * 64, 64)
        out_ref[pl.ds(at, 64)] = jnp.zeros((64, width), out_ref.dtype)
        return c

    lax.fori_loop(full, block // 64, blank, 0)


def solution(mesh):
    group = mesh.shape["g"]

    def local_part(keys_loc, rows_loc):
        n = keys_loc.shape[0]
        width = rows_loc.shape[1]
        full_cap = 2 * n // group
        cap = n // group + n // group // 64
        relay = LANES
        total = group * (cap + relay)
        vmem, smem, hbm = pltpu.VMEM, pltpu.SMEM, pl.ANY
        spec = lambda m: pl.BlockSpec(memory_space=m)
        me = lax.axis_index("g")
        run_rows = n // LANES

        sorted_keys, order = lax.sort((keys_loc, lax.iota(jnp.int32, n)), num_keys=1)
        windows, locs, rows3, table, idx1, idx2, info = pl.pallas_call(
            functools.partial(plan_kernel, group, n, cap, relay),
            out_shape=[
                jax.ShapeDtypeStruct((2 * run_rows, LANES), jnp.float32),
                jax.ShapeDtypeStruct((2 * run_rows, LANES), jnp.int32),
                jax.ShapeDtypeStruct((n, 2, LANES), rows_loc.dtype),
                jax.ShapeDtypeStruct((5, group, LANES), jnp.int32),
                jax.ShapeDtypeStruct((group, LANES), jnp.int32),
                jax.ShapeDtypeStruct((group, LANES), jnp.int32),
                jax.ShapeDtypeStruct((2,), jnp.int32),
            ],
            in_specs=[spec(vmem), spec(vmem)],
            out_specs=[spec(vmem)] * 6 + [spec(smem)],
            scratch_shapes=[
                pltpu.VMEM((group, run_rows + 24, LANES), jnp.float32),
                pltpu.SMEM((5, group, LANES), jnp.int32),
                pltpu.SemaphoreType.DMA((group,)),
                pltpu.SemaphoreType.DMA((group,)),
                pltpu.SemaphoreType.DMA,
            ],
            compiler_params=pltpu.CompilerParams(collective_id=0, has_side_effects=True, vmem_limit_bytes=40 << 20),
            name="plan",
        )(sorted_keys.reshape(run_rows, LANES), rows_loc)

        merged_keys, merged_loc = lax.sort((windows.reshape(-1), locs.reshape(-1)), num_keys=1)
        my_starts = lax.dynamic_index_in_dim(table[0], me, 0, keepdims=False)
        order_pad = jnp.concatenate([order, jnp.zeros((full_cap,), jnp.int32)])
        recv = pl.pallas_call(
            functools.partial(exchange_kernel, group, cap, relay, 16),
            out_shape=jax.ShapeDtypeStruct((total, 2, LANES), rows_loc.dtype),
            in_specs=[spec(smem)] * 4 + [spec(vmem)],
            out_specs=spec(vmem),
            scratch_shapes=[
                pltpu.VMEM((group, cap, 2, LANES), rows_loc.dtype),
                pltpu.VMEM((group, relay, 2, LANES), rows_loc.dtype),
                pltpu.VMEM((group, relay, 2, LANES), rows_loc.dtype),
                pltpu.VMEM((group * relay, 2, LANES), rows_loc.dtype),
                pltpu.SemaphoreType.DMA((2, group)),
                pltpu.SemaphoreType.DMA((2, group)),
                pltpu.SemaphoreType.DMA((2, group)),
            ],
            compiler_params=pltpu.CompilerParams(collective_id=1, has_side_effects=True, vmem_limit_bytes=40 << 20),
            name="exchange",
        )(order_pad, my_starts, idx1, idx2, rows3)

        block = 1024

        def placed(recv, merged_loc):
            return pl.pallas_call(
                functools.partial(place_kernel, block, 32),
                grid_spec=pltpu.PrefetchScalarGridSpec(
                    num_scalar_prefetch=2,
                    grid=(2 * n // block,),
                    in_specs=[spec(vmem)],
                    out_specs=pl.BlockSpec((block, width), lambda i, *_: (i, 0)),
                    scratch_shapes=[pltpu.VMEM((block, 2, LANES), rows_loc.dtype)],
                ),
                out_shape=jax.ShapeDtypeStruct((2 * n, width), rows_loc.dtype),
                compiler_params=pltpu.CompilerParams(vmem_limit_bytes=40 << 20),
                name="place",
            )(merged_loc, info, recv)

        def padded(recv, merged_loc):
            send_idx = jnp.concatenate([lax.dynamic_slice(order_pad, (my_starts[d],), (full_cap,)) for d in range(group)])
            send_rows = rows_loc[send_idx].reshape(group, full_cap, width)
            recv_rows = lax.all_to_all(send_rows, "g", 0, 0, tiled=True)
            slots = lax.iota(jnp.int32, 2 * n)
            _, merge_order = lax.sort((windows.reshape(-1), slots), num_keys=1)
            rows = recv_rows.reshape(-1, width)[merge_order]
            return jnp.where((slots < info[0])[:, None], rows, 0.0)

        merged_rows = lax.cond(info[1] == 1, placed, padded, recv, merged_loc)
        return merged_keys, merged_rows, info[0:1]

    row_spec = P(("batch", "g"))
    mat_spec = P(("batch", "g"), None)
    return jax.shard_map(local_part, mesh=mesh, in_specs=(row_spec, mat_spec), out_specs=(row_spec, mat_spec, row_spec), check_vma=False)
```

```python
import functools

import jax
import jax.numpy as jnp
from jax import lax
from jax.experimental import pallas as pl
from jax.experimental.pallas import tpu as pltpu
from jax.sharding import PartitionSpec as P

PAD_KEY = 128.0
LANES = 128
MESH = pl.DeviceIdType.MESH


def lane_prefix(x, lane):
    for step in (1, 2, 4):
        x = x + jnp.where(lane >= step, pltpu.roll(x, step, 1), 0)
    return x


def sub_prefix(x, sub):
    for step in (1, 2, 4):
        x = x + jnp.where(sub >= step, pltpu.roll(x, step, 0), 0)
    return x


def merge_runs(keys, locs, run_vregs):
    num = len(keys)
    sub = lax.broadcasted_iota(jnp.int32, keys[0].shape, 0)
    lane = lax.broadcasted_iota(jnp.int32, keys[0].shape, 1)
    size = 2 * run_vregs
    while size <= num:
        dist = size // 2
        while dist:
            for v in range(num):
                if v & dist:
                    continue
                a, b = (v, v + dist) if not v & size else (v + dist, v)
                swap = keys[b] < keys[a]
                keys[a], keys[b] = jnp.where(swap, keys[b], keys[a]), jnp.where(swap, keys[a], keys[b])
                locs[a], locs[b] = jnp.where(swap, locs[b], locs[a]), jnp.where(swap, locs[a], locs[b])
            dist //= 2
        for axis, index, extent, steps in ((0, sub, 8, (4, 2, 1)), (1, lane, LANES, (64, 32, 16, 8, 4, 2, 1))):
            for step in steps:
                bit = jnp.bitwise_and(index, step) != 0
                for v in range(num):
                    up = bit if not v & size else jnp.logical_not(bit)

                    def other(x):
                        return jnp.where(bit, pltpu.roll(x, step, axis), pltpu.roll(x, extent - step, axis))

                    peer_key, peer_loc = other(keys[v]), other(locs[v])
                    take = jnp.logical_xor(peer_key < keys[v], up)
                    keys[v] = jnp.where(take, peer_key, keys[v])
                    locs[v] = jnp.where(take, peer_loc, locs[v])
        size *= 2
    return keys, locs


def exchange_kernel(group, n, cap, relay, unroll, keys_ref, order_ref, rows_ref,
                    out_ref, mkey_ref, mloc_ref, win_ref, start_ref, info_ref,
                    all_keys, rows3, near, far1, far2, got, tab_ref, idx1_ref, idx2_ref,
                    tab, order, idx1_sm, idx2_sm,
                    key_sems, near_sems, far1_sems, far2_sems, local_sems):
    run_rows = n // LANES
    win_rows = 2 * run_rows // group
    me = lax.axis_index("g")
    order_copy = pltpu.make_async_copy(order_ref, order.at[pl.ds(0, n)], local_sems.at[0])
    tail_copy = pltpu.make_async_copy(
        order_ref.at[pl.ds(0, order.shape[0] - n)], order.at[pl.ds(n, order.shape[0] - n)], local_sems.at[1])
    order_copy.start()
    tail_copy.start()
    barrier = pltpu.get_barrier_semaphore()
    for off in range(1, group):
        pl.semaphore_signal(barrier, inc=1, device_id={"g": lax.rem(me + off, group)}, device_id_type=MESH)

    def relayout(t, c):
        at = pl.multiple_of(t * 64, 64)
        rows3[pl.ds(at, 64)] = rows_ref[pl.ds(at, 64)].reshape(64, 2, LANES)
        return c

    lax.fori_loop(0, n // 192, relayout, 0)
    pl.semaphore_wait(barrier, group - 1)

    def send(src, dst, sems, off):
        copy = pltpu.make_async_remote_copy(
            src_ref=src, dst_ref=dst, send_sem=sems.at[0, off], recv_sem=sems.at[1, off],
            device_id={"g": lax.rem(me + off, group)}, device_id_type=MESH)
        copy.start()
        return copy

    copies = [send(keys_ref, all_keys.at[me, pl.ds(0, run_rows)], key_sems, off) for off in range(1, group)]
    all_keys[me, pl.ds(0, run_rows)] = keys_ref[...]
    tail = all_keys.shape[1] - run_rows
    for s in range(group):
        all_keys[s, pl.ds(run_rows, tail)] = jnp.full((tail, LANES), PAD_KEY, jnp.float32)
    lax.fori_loop(n // 192, n // 64, relayout, 0)
    for copy in copies:
        copy.wait()

    count = group * group
    stride = run_rows // group
    col = jnp.concatenate(
        [jnp.concatenate([all_keys[s, pl.ds(m * stride, 1)] for m in range(group)], axis=0) for s in range(group)], axis=0)
    col = jnp.broadcast_to(col[:, 0:1], (count, LANES))
    r_id = lax.broadcasted_iota(jnp.int32, (count, LANES), 0)
    l_id = lax.broadcasted_iota(jnp.int32, (count, LANES), 1)
    row = jnp.sum(jnp.where(r_id == l_id, col, 0.0), axis=0, keepdims=True)
    less = (jnp.broadcast_to(row, (count, LANES)) < col) & (l_id < count)
    rank = jnp.sum(jnp.where(less, 1.0, 0.0), axis=1, keepdims=True)
    want = (group * l_id + group // 2).astype(jnp.float32)
    splitters = jnp.sum(jnp.where(jnp.broadcast_to(rank, (count, LANES)) == want, col, 0.0), axis=0, keepdims=True)

    lane = lax.broadcasted_iota(jnp.int32, (group, LANES), 1)
    sub = lax.broadcasted_iota(jnp.int32, (group, LANES), 0)
    edges = jnp.where(lane < group, 0, n)
    for j in range(1, group):
        part = []
        for s in range(group):
            hit = jnp.where(all_keys[s, pl.ds(0, run_rows)] < splitters[0, j], 1, 0)
            part.append(jnp.sum(hit, axis=0, keepdims=True))
        total = jnp.sum(jnp.concatenate(part, axis=0), axis=1, keepdims=True)
        edges = jnp.where(lane == j, jnp.broadcast_to(total, (group, LANES)), edges)
    counts = jnp.where(lane < group, pltpu.roll(edges, LANES - 1, 1) - edges, 0)
    over = jnp.maximum(counts - cap, 0)
    share = jnp.right_shift(over + (group - 1), group.bit_length() - 1)
    first = lane_prefix(share, lane) - share
    second = sub_prefix(share, sub) - share
    worst = jnp.maximum(jnp.max(first + share), jnp.max(second + share))
    for t, x in enumerate((edges, counts, share, first, second)):
        tab_ref[t] = x
    to_smem = pltpu.make_async_copy(tab_ref, tab, local_sems.at[2])
    to_smem.start()
    order_copy.wait()
    tail_copy.wait()
    to_smem.wait()

    idx1 = jnp.zeros((group, LANES), jnp.int32)
    for j in range(group):
        q, a = tab[2, me, j], tab[3, me, j]
        src = tab[0, me, j] + cap - a + q * sub + lane
        idx1 = jnp.where((lane >= a) & (lane < a + q), src, idx1)
    idx1_ref[...] = jnp.clip(idx1, 0, n - 1)
    idx1_copy = pltpu.make_async_copy(idx1_ref, idx1_sm, local_sems.at[3])
    idx1_copy.start()

    def gather(dst, base, size, pick):
        def step(t, c):
            for u in range(unroll):
                dst[base + t * unroll + u] = pick(t * unroll, u)
            return c
        lax.fori_loop(0, size // unroll, step, 0)

    waits, firsts = [], []

    def direct(off):
        start = tab[0, me, lax.rem(me + off, group)]

        def pick(at, u):
            return rows3[order[(start + at) + u]]

        if off:
            gather(near.at[off], 0, cap, pick)
            waits.append(send(near.at[off], out_ref.at[pl.ds(me * cap, cap)], near_sems, off))
        else:
            gather(out_ref, me * cap, cap, pick)

    offsets = [2, 6, 4, 3, 7, 5, 1, 0]
    for off in offsets[:3]:
        direct(off)
    idx1_copy.wait()
    for off in offsets:
        peer = lax.rem(me + off, group)

        def pick(at, u):
            return rows3[order[idx1_sm[peer, at + u]]]

        if off:
            gather(far1.at[off], 0, relay, pick)
            firsts.append(send(far1.at[off], got.at[pl.ds(me * relay, relay)], far1_sems, off))
        else:
            gather(got, me * relay, relay, pick)
    for off in offsets[3:]:
        direct(off)

    lane1 = lane[0:1]
    for j in range(group):
        line = jnp.zeros((1, LANES), jnp.int32)
        for s in range(group):
            q, a, b = tab[2, s, j], tab[3, s, j], tab[4, s, j]
            line = jnp.where((lane1 >= b) & (lane1 < b + q), s * relay + a - b + lane1, line)
        idx2_ref[pl.ds(j, 1)] = jnp.clip(line, 0, group * relay - 1)
    idx2_copy = pltpu.make_async_copy(idx2_ref, idx2_sm, local_sems.at[4])
    idx2_copy.start()

    wl = lax.broadcasted_iota(jnp.int32, (win_rows, LANES), 1)
    pos = lax.broadcasted_iota(jnp.int32, (win_rows, LANES), 0) * LANES + wl
    own = jnp.int32(0)
    run_keys, run_locs = [], []
    for s in range(group):
        start, num = tab[0, s, me], tab[1, s, me]
        q, b = tab[2, s, me], tab[4, s, me]
        own = own + num
        shift = jnp.bitwise_and(start, LANES - 1)
        at = jnp.right_shift(start, LANES.bit_length() - 1)
        turn = jnp.bitwise_and(LANES - shift, LANES - 1)
        one = pltpu.roll(all_keys[s, pl.ds(at, win_rows)], turn, 1)
        two = pltpu.roll(all_keys[s, pl.ds(at + 1, win_rows)], turn, 1)
        window = jnp.where(pos < num, jnp.where(wl < LANES - shift, one, two), PAD_KEY)
        win_ref[pl.ds(s * win_rows, win_rows)] = window
        where = pos
        if s % 2:
            window = jnp.take_along_axis(window, LANES - 1 - wl, axis=1)
            window = jnp.concatenate([window[r:r + 1] for r in range(win_rows - 1, -1, -1)], axis=0)
            where = win_rows * LANES - 1 - pos
        extra = where - cap
        far = group * cap + b + extra
        for m in range(1, group):
            far = far + jnp.where(extra >= m * q, relay - q, 0)
        loc = jnp.where(where < cap, s * cap + where, far)
        loc = jnp.where(where < num, jnp.clip(loc, 0, group * (cap + relay) - 1), 0)
        for v in range(win_rows // 8):
            run_keys.append(window[v * 8:v * 8 + 8])
            run_locs.append(loc[v * 8:v * 8 + 8])
    info_ref[0] = own
    info_ref[1] = jnp.where(worst <= relay, 0, 1)
    for j in range(group):
        start_ref[j] = tab[0, me, j]
    merged, placed = merge_runs(run_keys, run_locs, win_rows // 8)
    for v in range(2 * run_rows // 8):
        mkey_ref[pl.ds(v * 8, 8)] = merged[v]
        mloc_ref[pl.ds(v * 8, 8)] = placed[v]

    idx2_copy.wait()
    for copy in firsts:
        copy.wait()
    base2 = group * cap + me * relay
    for off in offsets:
        peer = lax.rem(me + off, group)

        def pick(at, u):
            return got[idx2_sm[peer, at + u]]

        if off:
            gather(far2.at[off], 0, relay, pick)
            waits.append(send(far2.at[off], out_ref.at[pl.ds(base2, relay)], far2_sems, off))
        else:
            gather(out_ref, base2, relay, pick)
    for copy in waits:
        copy.wait()


def place_kernel(block, chunk, loc_ref, info_ref, rows_ref, out_ref, tmp_a, tmp_b):
    base = pl.program_id(0) * block
    num = jnp.clip(info_ref[0] - base, 0, block)
    width = out_ref.shape[1]

    def fetch(c, tmp):
        at = base + c * chunk
        for u in range(chunk):
            tmp[u] = rows_ref[loc_ref[at + u]]

    def finish(c, tmp):
        at = pl.multiple_of(c * chunk, chunk)
        out_ref[pl.ds(at, chunk)] = tmp[...].reshape(chunk, width)

    pairs = (num + 2 * chunk - 1) // (2 * chunk)

    @pl.when(pairs > 0)
    def _():
        fetch(0, tmp_a)

        def step(t, c):
            fetch(2 * t + 1, tmp_b)
            finish(2 * t, tmp_a)
            fetch(jnp.minimum(2 * t + 2, block // chunk - 1), tmp_a)
            finish(2 * t + 1, tmp_b)
            return c

        lax.fori_loop(0, pairs, step, 0)
        edge = jnp.minimum(num // chunk, block // chunk - 1)
        at = pl.multiple_of(edge * chunk, chunk)
        row = at + lax.broadcasted_iota(jnp.int32, (chunk, width), 0)
        x = out_ref[pl.ds(at, chunk)]
        out_ref[pl.ds(at, chunk)] = jnp.where(row < num, x, jnp.zeros_like(x))

    def blank(t, c):
        at = pl.multiple_of(t * chunk, chunk)
        out_ref[pl.ds(at, chunk)] = jnp.zeros((chunk, width), out_ref.dtype)
        return c

    lax.fori_loop((num + chunk - 1) // chunk, block // chunk, blank, 0)


def solution(mesh):
    group = mesh.shape["g"]

    def local_part(keys_loc, rows_loc):
        n = keys_loc.shape[0]
        width = rows_loc.shape[1]
        full_cap = 2 * n // group
        cap = n // group + n // group // 64
        relay = LANES
        total = group * (cap + relay)
        spec = lambda m: pl.BlockSpec(memory_space=m)
        vmem, smem = pltpu.VMEM, pltpu.SMEM
        dtype = rows_loc.dtype
        run_rows = n // LANES
        pad = -(-cap // LANES) * LANES

        sorted_keys, order = lax.sort((keys_loc, lax.iota(jnp.int32, n)), num_keys=1)
        recv, merged_keys, merged_loc, windows, my_starts, info = pl.pallas_call(
            functools.partial(exchange_kernel, group, n, cap, relay, 16),
            out_shape=[
                jax.ShapeDtypeStruct((total, 2, LANES), dtype),
                jax.ShapeDtypeStruct((2 * run_rows, LANES), jnp.float32),
                jax.ShapeDtypeStruct((2 * run_rows, LANES), jnp.int32),
                jax.ShapeDtypeStruct((2 * run_rows, LANES), jnp.float32),
                jax.ShapeDtypeStruct((group,), jnp.int32),
                jax.ShapeDtypeStruct((2,), jnp.int32),
            ],
            in_specs=[spec(vmem), spec(pl.ANY), spec(vmem)],
            out_specs=[spec(vmem)] * 4 + [spec(smem)] * 2,
            scratch_shapes=[
                pltpu.VMEM((group, run_rows + 24, LANES), jnp.float32),
                pltpu.VMEM((n, 2, LANES), dtype),
                pltpu.VMEM((group, cap, 2, LANES), dtype),
                pltpu.VMEM((group, relay, 2, LANES), dtype),
                pltpu.VMEM((group, relay, 2, LANES), dtype),
                pltpu.VMEM((group * relay, 2, LANES), dtype),
                pltpu.VMEM((5, group, LANES), jnp.int32),
                pltpu.VMEM((group, LANES), jnp.int32),
                pltpu.VMEM((group, LANES), jnp.int32),
                pltpu.SMEM((5, group, LANES), jnp.int32),
                pltpu.SMEM((n + pad,), jnp.int32),
                pltpu.SMEM((group, LANES), jnp.int32),
                pltpu.SMEM((group, LANES), jnp.int32),
            ] + [pltpu.SemaphoreType.DMA((2, group))] * 4 + [pltpu.SemaphoreType.DMA((5,))],
            compiler_params=pltpu.CompilerParams(collective_id=0, has_side_effects=True, vmem_limit_bytes=32 << 20),
            name="exchange",
        )(sorted_keys.reshape(run_rows, LANES), order, rows_loc)

        block = 2048
        chunk = 64
        merged_rows = pl.pallas_call(
            functools.partial(place_kernel, block, chunk),
            grid_spec=pltpu.PrefetchScalarGridSpec(
                num_scalar_prefetch=2,
                grid=(2 * n // block,),
                in_specs=[spec(vmem)],
                out_specs=pl.BlockSpec((block, width), lambda i, *_: (i, 0)),
                scratch_shapes=[pltpu.VMEM((chunk, 2, LANES), dtype)] * 2,
            ),
            out_shape=jax.ShapeDtypeStruct((2 * n, width), dtype),
            compiler_params=pltpu.CompilerParams(vmem_limit_bytes=24 << 20),
            name="place",
        )(merged_loc.reshape(-1), info, recv)

        merged_rows, windows, my_starts, info = lax.optimization_barrier((merged_rows, windows, my_starts, info))

        def padded(carry):
            left, _ = carry
            order_pad = jnp.concatenate([order, jnp.zeros((full_cap,), jnp.int32)])
            at = my_starts + (left - 1)
            send_idx = jnp.concatenate([lax.dynamic_slice(order_pad, (at[d],), (full_cap,)) for d in range(group)])
            send_rows = rows_loc[send_idx].reshape(group, full_cap, width)
            recv_rows = lax.all_to_all(send_rows, "g", 0, 0, tiled=True)
            slots = lax.iota(jnp.int32, 2 * n)
            _, merge_order = lax.sort((windows.reshape(-1), slots), num_keys=1)
            rows = recv_rows.reshape(-1, width)[merge_order]
            return left - 1, jnp.where((slots < info[0])[:, None], rows, 0.0)

        _, merged_rows = lax.while_loop(lambda carry: carry[0] > 0, padded, (info[1], merged_rows))
        return merged_keys.reshape(-1), merged_rows, info[0:1]

    row_spec = P(("batch", "g"))
    mat_spec = P(("batch", "g"), None)
    return jax.shard_map(local_part, mesh=mesh, in_specs=(row_spec, mat_spec), out_specs=(row_spec, mat_spec, row_spec), check_vma=False)
```

```python
import functools

import jax
import jax.numpy as jnp
from jax import lax
from jax.experimental import pallas as pl
from jax.experimental.pallas import tpu as pltpu
from jax.sharding import PartitionSpec as P

PAD_KEY = 128.0
LANES = 128
MESH = pl.DeviceIdType.MESH


def lane_prefix(x, lane):
    for step in (1, 2, 4):
        x = x + jnp.where(lane >= step, pltpu.roll(x, step, 1), 0)
    return x


def sub_prefix(x, sub):
    for step in (1, 2, 4):
        x = x + jnp.where(sub >= step, pltpu.roll(x, step, 0), 0)
    return x


def merge_runs(keys, locs, run_vregs):
    num = len(keys)
    sub = lax.broadcasted_iota(jnp.int32, keys[0].shape, 0)
    lane = lax.broadcasted_iota(jnp.int32, keys[0].shape, 1)
    size = 2 * run_vregs
    while size <= num:
        dist = size // 2
        while dist:
            for v in range(num):
                if v & dist:
                    continue
                a, b = (v, v + dist) if not v & size else (v + dist, v)
                swap = keys[b] < keys[a]
                keys[a], keys[b] = jnp.where(swap, keys[b], keys[a]), jnp.where(swap, keys[a], keys[b])
                locs[a], locs[b] = jnp.where(swap, locs[b], locs[a]), jnp.where(swap, locs[a], locs[b])
            dist //= 2
        for axis, index, extent, steps in ((0, sub, 8, (4, 2, 1)), (1, lane, LANES, (64, 32, 16, 8, 4, 2, 1))):
            for step in steps:
                bit = jnp.bitwise_and(index, step) != 0
                for v in range(num):
                    up = bit if not v & size else jnp.logical_not(bit)

                    def other(x):
                        return jnp.where(bit, pltpu.roll(x, step, axis), pltpu.roll(x, extent - step, axis))

                    peer_key, peer_loc = other(keys[v]), other(locs[v])
                    take = jnp.logical_xor(peer_key < keys[v], up)
                    keys[v] = jnp.where(take, peer_key, keys[v])
                    locs[v] = jnp.where(take, peer_loc, locs[v])
        size *= 2
    return keys, locs


def exchange_kernel(group, n, cap, relay, pieces, keys_ref, order_ref, rows_hbm,
                    out_ref, mkey_ref, mloc_ref, win_ref, start_ref, own_ref, need_ref,
                    rows_ref, keys_pad, sample, samples, outbox, inbox, rows3, near, far1, far2, got, tab_ref, idx1_ref, idx2_ref,
                    tab, order, idx1_sm, idx2_sm, edge_sm,
                    sample_sems, box_sems, near_sems, half_sems, far1_sems, far2_sems, local_sems, load_sems):
    run_rows = n // LANES
    win_rows = 2 * run_rows // group
    box_rows = win_rows + 8
    me = lax.axis_index("g")
    order_copy = pltpu.make_async_copy(order_ref, order.at[pl.ds(0, n)], local_sems.at[0])
    tail_copy = pltpu.make_async_copy(
        order_ref.at[pl.ds(0, order.shape[0] - n)], order.at[pl.ds(n, order.shape[0] - n)], local_sems.at[1])
    order_copy.start()
    tail_copy.start()
    barrier = pltpu.get_barrier_semaphore()
    for off in range(1, group):
        pl.semaphore_signal(barrier, inc=1, device_id={"g": lax.rem(me + off, group)}, device_id_type=MESH)

    piece = n // pieces
    loads = []
    for p in range(pieces):
        at = pl.ds(p * piece, piece)
        loads.append(pltpu.make_async_copy(rows_hbm.at[at], rows_ref.at[at], load_sems.at[p]))
        loads[p].start()
    stride = run_rows // group
    sample[...] = jnp.concatenate([keys_ref[pl.ds(m * stride, 1)] for m in range(group)], axis=0)
    samples[me] = jnp.concatenate([keys_ref[pl.ds(m * stride, 1)] for m in range(group)], axis=0)
    keys_pad[pl.ds(0, run_rows)] = keys_ref[...]
    tail = keys_pad.shape[0] - run_rows
    keys_pad[pl.ds(run_rows, tail)] = jnp.full((tail, LANES), PAD_KEY, jnp.float32)

    def relayout(t, c):
        at = pl.multiple_of(t * 64, 64)
        rows3[pl.ds(at, 64)] = rows_ref[pl.ds(at, 64)].reshape(64, 2, LANES)
        return c

    def ready(lo, hi):
        for p in range(lo, hi):
            loads[p].wait()
            lax.fori_loop(p * piece // 64, (p + 1) * piece // 64, relayout, 0)

    ready(0, pieces // 2)
    pl.semaphore_wait(barrier, group - 1)

    def send(src, dst, sems, off):
        copy = pltpu.make_async_remote_copy(
            src_ref=src, dst_ref=dst, send_sem=sems.at[0, off], recv_sem=sems.at[1, off],
            device_id={"g": lax.rem(me + off, group)}, device_id_type=MESH)
        copy.start()
        return copy

    offsets = [2, 6, 4, 3, 7, 5, 1, 0]
    copies = [send(sample, samples.at[me], sample_sems, off) for off in offsets[:-1]]
    ready(pieces // 2, pieces)
    for copy in copies:
        copy.wait()

    count = group * group
    col = jnp.broadcast_to(samples[...].reshape(count, LANES)[:, 0:1], (count, LANES))
    r_id = lax.broadcasted_iota(jnp.int32, (count, LANES), 0)
    l_id = lax.broadcasted_iota(jnp.int32, (count, LANES), 1)
    row = jnp.sum(jnp.where(r_id == l_id, col, 0.0), axis=0, keepdims=True)
    less = (jnp.broadcast_to(row, (count, LANES)) < col) & (l_id < count)
    rank = jnp.sum(jnp.where(less, 1.0, 0.0), axis=1, keepdims=True)
    want = (group * l_id + group // 2).astype(jnp.float32)
    splitters = jnp.sum(jnp.where(jnp.broadcast_to(rank, (count, LANES)) == want, col, 0.0), axis=0, keepdims=True)
    below = [jnp.zeros((1, LANES), jnp.int32)]
    for j in range(1, group):
        below.append(jnp.sum(jnp.where(keys_ref[...] < splitters[0, j], 1, 0), axis=0, keepdims=True))
    below = jnp.sum(jnp.concatenate(below, axis=0), axis=1, keepdims=True)
    edges = [jnp.clip(below[j, 0], 0, n) for j in range(group)] + [jnp.int32(n)]

    lane = lax.broadcasted_iota(jnp.int32, (group, LANES), 1)
    sub = lax.broadcasted_iota(jnp.int32, (group, LANES), 0)
    mine = jnp.zeros((8, LANES), jnp.int32)
    for j in range(group):
        edge_sm[j] = edges[j]
        start_ref[j] = edges[j]
        mine = jnp.where(lane == j, edges[j + 1] - edges[j], mine)
    edge_sm[group] = edges[group]
    mine = mine.astype(jnp.float32)
    wl = lax.broadcasted_iota(jnp.int32, (win_rows, LANES), 1)
    pos = lax.broadcasted_iota(jnp.int32, (win_rows, LANES), 0) * LANES + wl
    for off in offsets:
        peer = lax.rem(me + off, group)
        start = edge_sm[peer]
        shift = jnp.bitwise_and(start, LANES - 1)
        at = jnp.clip(jnp.right_shift(start, LANES.bit_length() - 1), 0, run_rows)
        turn = jnp.bitwise_and(LANES - shift, LANES - 1)
        one = pltpu.roll(keys_pad[pl.ds(at, win_rows)], turn, 1)
        two = pltpu.roll(keys_pad[pl.ds(at + 1, win_rows)], turn, 1)
        window = jnp.where(pos < edge_sm[peer + 1] - start, jnp.where(wl < LANES - shift, one, two), PAD_KEY)
        if off:
            outbox[off, pl.ds(0, win_rows)] = window
            outbox[off, pl.ds(win_rows, 8)] = mine
        else:
            inbox[me, pl.ds(0, win_rows)] = window
            inbox[me, pl.ds(win_rows, 8)] = mine
    copies = [send(outbox.at[off], inbox.at[me], box_sems, off) for off in offsets[:-1]]
    order_copy.wait()
    tail_copy.wait()

    def gather(dst, base, size, pick):
        unroll = next(u for u in (40, 32, 16) if size % u == 0)

        def step(t, c):
            for u in range(unroll):
                dst[base + t * unroll + u] = pick(t * unroll, u)
            return c
        lax.fori_loop(0, size // unroll, step, 0)

    waits, firsts = [], []

    def direct(off, low=0, high=cap, sems=near_sems):
        start = edge_sm[lax.rem(me + off, group)] + low

        def pick(at, u):
            return rows3[order[(start + at) + u]]

        size = high - low
        if off:
            gather(near.at[off], low, size, pick)
            waits.append(send(near.at[off, pl.ds(low, size)], out_ref.at[pl.ds(me * cap + low, size)], sems, off))
        else:
            gather(out_ref, me * cap + low, size, pick)

    early = cap // 80 * 40
    for off in offsets[:2]:
        direct(off, 0, early, half_sems)
    for off in offsets[:2]:
        direct(off, early, cap)
    direct(offsets[2])
    for copy in copies:
        copy.wait()
    counts = jnp.concatenate([inbox[s, pl.ds(win_rows, 1)] for s in range(group)], axis=0).astype(jnp.int32)
    counts = jnp.clip(counts, 0, n)
    over = jnp.maximum(counts - cap, 0)
    share = jnp.right_shift(over + (group - 1), group.bit_length() - 1)
    first = lane_prefix(share, lane) - share
    second = sub_prefix(share, sub) - share
    worst = jnp.maximum(jnp.max(first + share), jnp.max(second + share))
    for t, x in enumerate((counts, share, first, second)):
        tab_ref[t] = x
    to_smem = pltpu.make_async_copy(tab_ref, tab, local_sems.at[2])
    to_smem.start()
    direct(offsets[3])
    to_smem.wait()
    idx1 = jnp.zeros((group, LANES), jnp.int32)
    for j in range(group):
        q, a = tab[1, me, j], tab[2, me, j]
        src = edge_sm[j] + cap - a + q * sub + lane
        idx1 = jnp.where((lane >= a) & (lane < a + q), src, idx1)
    idx1_ref[...] = jnp.clip(idx1, 0, n - 1)
    idx1_copy = pltpu.make_async_copy(idx1_ref, idx1_sm, local_sems.at[3])
    idx1_copy.start()
    direct(offsets[4])
    idx1_copy.wait()
    for off in offsets:
        peer = lax.rem(me + off, group)

        def pick(at, u):
            return rows3[order[idx1_sm[peer, at + u]]]

        if off:
            gather(far1.at[off], 0, relay, pick)
            firsts.append(send(far1.at[off], got.at[pl.ds(me * relay, relay)], far1_sems, off))
        else:
            gather(got, me * relay, relay, pick)
    for off in offsets[5:]:
        direct(off)

    lane1 = lane[0:1]
    for j in range(group):
        line = jnp.zeros((1, LANES), jnp.int32)
        for s in range(group):
            q, a, b = tab[1, s, j], tab[2, s, j], tab[3, s, j]
            line = jnp.where((lane1 >= b) & (lane1 < b + q), s * relay + a - b + lane1, line)
        idx2_ref[pl.ds(j, 1)] = jnp.clip(line, 0, group * relay - 1)
    idx2_copy = pltpu.make_async_copy(idx2_ref, idx2_sm, local_sems.at[4])
    idx2_copy.start()

    own = jnp.int32(0)
    run_keys, run_locs = [], []
    for s in range(group):
        num, q, b = tab[0, s, me], tab[1, s, me], tab[3, s, me]
        own = own + num
        window = inbox[s, pl.ds(0, win_rows)]
        win_ref[pl.ds(s * win_rows, win_rows)] = window
        where = pos
        if s % 2:
            window = jnp.take_along_axis(window, LANES - 1 - wl, axis=1)
            window = jnp.concatenate([window[r:r + 1] for r in range(win_rows - 1, -1, -1)], axis=0)
            where = win_rows * LANES - 1 - pos
        extra = where - cap
        far = group * cap + b + extra
        for m in range(1, group):
            far = far + jnp.where(extra >= m * q, relay - q, 0)
        loc = jnp.where(where < cap, s * cap + where, far)
        loc = jnp.where(where < num, jnp.clip(loc, 0, group * (cap + relay) - 1), 0)
        for v in range(win_rows // 8):
            run_keys.append(window[v * 8:v * 8 + 8])
            run_locs.append(loc[v * 8:v * 8 + 8])
    own_ref[0] = own
    need_ref[0] = jnp.where(worst <= relay, 0, 1)
    merged, placed = merge_runs(run_keys, run_locs, win_rows // 8)
    for v in range(2 * run_rows // 8):
        mkey_ref[pl.ds(v * 8, 8)] = merged[v]
        mloc_ref[pl.ds(v * 8, 8)] = placed[v]

    idx2_copy.wait()
    for copy in firsts:
        copy.wait()
    base2 = group * cap + me * relay
    for off in offsets:
        peer = lax.rem(me + off, group)

        def pick(at, u):
            return got[idx2_sm[peer, at + u]]

        if off:
            gather(far2.at[off], 0, relay, pick)
            waits.append(send(far2.at[off], out_ref.at[pl.ds(base2, relay)], far2_sems, off))
        else:
            gather(out_ref, base2, relay, pick)
    for copy in waits:
        copy.wait()


def place_kernel(block, chunk, loc_ref, own_ref, rows_ref, keys_ref, out_ref, out_own_ref, out_keys_ref,
                 loc, bufs, blanks, tmp_a, tmp_b, loc_sems, out_sems, blank_sems, key_sem):
    blocks = out_ref.shape[0] // block
    width = out_ref.shape[1]
    own = jnp.clip(own_ref[0], 0, out_ref.shape[0])
    out_own_ref[0] = own
    used = (own + block - 1) // block

    def loc_copy(b):
        at = pl.ds(pl.multiple_of(b * block, block), block)
        return pltpu.make_async_copy(loc_ref.at[at], loc.at[at], loc_sems.at[b])

    def out_copy(b, src, sem):
        return pltpu.make_async_copy(src, out_ref.at[pl.ds(pl.multiple_of(b * block, block), block)], sem)

    for b in range(blocks):
        loc_copy(b).start()
    keys_copy = pltpu.make_async_copy(keys_ref, out_keys_ref, key_sem)
    keys_copy.start()
    blanks[...] = jnp.zeros_like(blanks)

    def blank(b, c):
        out_copy(b, blanks, blank_sems.at[b]).start()
        return c

    lax.fori_loop(used, blocks, blank, 0)

    def fetch(base, tmp):
        for u in range(chunk):
            tmp[u] = rows_ref[loc[base + u]]

    def one_block(b, carry):
        slot = lax.rem(b, 2)
        base = b * block
        num = jnp.minimum(own - base, block)
        loc_copy(b).wait()

        @pl.when(b >= 2)
        def _():
            out_copy(b - 2, bufs.at[slot], out_sems.at[slot]).wait()

        def finish(c, tmp):
            bufs[slot, pl.ds(pl.multiple_of(c * chunk, chunk), chunk)] = tmp[...].reshape(chunk, width)

        fetch(base, tmp_a)

        def step(t, c):
            fetch(base + (2 * t + 1) * chunk, tmp_b)
            finish(2 * t, tmp_a)
            fetch(base + jnp.minimum(2 * t + 2, block // chunk - 1) * chunk, tmp_a)
            finish(2 * t + 1, tmp_b)
            return c

        lax.fori_loop(0, (num + 2 * chunk - 1) // (2 * chunk), step, 0)

        @pl.when(num < block)
        def _():
            edge = num // chunk
            at = pl.multiple_of(edge * chunk, chunk)
            row = at + lax.broadcasted_iota(jnp.int32, (chunk, width), 0)
            x = bufs[slot, pl.ds(at, chunk)]
            bufs[slot, pl.ds(at, chunk)] = jnp.where(row < num, x, jnp.zeros_like(x))

            def clear(t, c):
                bufs[slot, pl.ds(pl.multiple_of(t * chunk, chunk), chunk)] = jnp.zeros((chunk, width), bufs.dtype)
                return c

            lax.fori_loop(edge + 1, block // chunk, clear, 0)

        out_copy(b, bufs.at[slot], out_sems.at[slot]).start()
        return carry

    lax.fori_loop(0, used, one_block, 0)
    for back in (2, 1):
        @pl.when(used >= back)
        def _():
            b = used - back
            slot = lax.rem(b, 2)
            out_copy(b, bufs.at[slot], out_sems.at[slot]).wait()

    keys_copy.wait()

    def settle(b, c):
        out_copy(b, blanks, blank_sems.at[b]).wait()
        return c

    lax.fori_loop(used, blocks, settle, 0)

    def skip(b, c):
        loc_copy(b).wait()
        return c

    lax.fori_loop(used, blocks, skip, 0)


def solution(mesh):
    group = mesh.shape["g"]

    def local_part(keys_loc, rows_loc):
        n = keys_loc.shape[0]
        width = rows_loc.shape[1]
        full_cap = 2 * n // group
        cap = n // group + n // group // 64
        relay = LANES
        total = group * (cap + relay)
        spec = lambda m: pl.BlockSpec(memory_space=m)
        vmem, smem = pltpu.VMEM, pltpu.SMEM
        dtype = rows_loc.dtype
        run_rows = n // LANES
        pad = -(-cap // LANES) * LANES

        sorted_keys, order = lax.sort((keys_loc, lax.iota(jnp.int32, n)), num_keys=1)
        recv, merged_keys, merged_loc, windows, my_starts, own, need = pl.pallas_call(
            functools.partial(exchange_kernel, group, n, cap, relay, 8),
            out_shape=[
                jax.ShapeDtypeStruct((total, 2, LANES), dtype),
                jax.ShapeDtypeStruct((2 * run_rows, LANES), jnp.float32),
                jax.ShapeDtypeStruct((2 * run_rows, LANES), jnp.int32),
                jax.ShapeDtypeStruct((2 * run_rows, LANES), jnp.float32),
                jax.ShapeDtypeStruct((group,), jnp.int32),
                jax.ShapeDtypeStruct((1,), jnp.int32),
                jax.ShapeDtypeStruct((1,), jnp.int32),
            ],
            in_specs=[spec(vmem), spec(pl.ANY), spec(pl.ANY)],
            out_specs=[spec(vmem)] * 4 + [spec(smem)] * 3,
            scratch_shapes=[
                pltpu.VMEM((n, width), dtype),
                pltpu.VMEM((run_rows + 24, LANES), jnp.float32),
                pltpu.VMEM((group, LANES), jnp.float32),
                pltpu.VMEM((group, group, LANES), jnp.float32),
                pltpu.VMEM((group, 2 * run_rows // group + 8, LANES), jnp.float32),
                pltpu.VMEM((group, 2 * run_rows // group + 8, LANES), jnp.float32),
                pltpu.VMEM((n, 2, LANES), dtype),
                pltpu.VMEM((group, cap, 2, LANES), dtype),
                pltpu.VMEM((group, relay, 2, LANES), dtype),
                pltpu.VMEM((group, relay, 2, LANES), dtype),
                pltpu.VMEM((group * relay, 2, LANES), dtype),
                pltpu.VMEM((4, group, LANES), jnp.int32),
                pltpu.VMEM((group, LANES), jnp.int32),
                pltpu.VMEM((group, LANES), jnp.int32),
                pltpu.SMEM((4, group, LANES), jnp.int32),
                pltpu.SMEM((n + pad,), jnp.int32),
                pltpu.SMEM((group, LANES), jnp.int32),
                pltpu.SMEM((group, LANES), jnp.int32),
                pltpu.SMEM((group + 1,), jnp.int32),
            ] + [pltpu.SemaphoreType.DMA((2, group))] * 6 + [pltpu.SemaphoreType.DMA((5,)), pltpu.SemaphoreType.DMA((8,))],
            compiler_params=pltpu.CompilerParams(collective_id=0, has_side_effects=True, vmem_limit_bytes=32 << 20),
            name="exchange",
        )(sorted_keys.reshape(run_rows, LANES), order, rows_loc)

        block = 1024
        chunk = 64
        blocks = 2 * n // block
        merged_rows, counts, sorted_out = pl.pallas_call(
            functools.partial(place_kernel, block, chunk),
            out_shape=[
                jax.ShapeDtypeStruct((2 * n, width), dtype),
                jax.ShapeDtypeStruct((1,), jnp.int32),
                jax.ShapeDtypeStruct((2 * run_rows, LANES), jnp.float32),
            ],
            in_specs=[spec(pl.ANY), spec(smem), spec(vmem), spec(vmem)],
            out_specs=[spec(pl.ANY), spec(smem), spec(pl.ANY)],
            scratch_shapes=[
                pltpu.SMEM((2 * n,), jnp.int32),
                pltpu.VMEM((2, block, width), dtype),
                pltpu.VMEM((block, width), dtype),
                pltpu.VMEM((chunk, 2, LANES), dtype),
                pltpu.VMEM((chunk, 2, LANES), dtype),
                pltpu.SemaphoreType.DMA((blocks,)),
                pltpu.SemaphoreType.DMA((2,)),
                pltpu.SemaphoreType.DMA((blocks,)),
                pltpu.SemaphoreType.DMA,
            ],
            compiler_params=pltpu.CompilerParams(vmem_limit_bytes=16 << 20),
            name="place",
        )(merged_loc.reshape(-1), own, recv, merged_keys)

        merged_rows, windows, my_starts, need = lax.optimization_barrier((merged_rows, windows, my_starts, need))

        def padded(carry):
            left, _ = carry
            order_pad = jnp.concatenate([order, jnp.zeros((full_cap,), jnp.int32)])
            at = my_starts + (left - 1)
            send_idx = jnp.concatenate([lax.dynamic_slice(order_pad, (at[d],), (full_cap,)) for d in range(group)])
            send_rows = rows_loc[send_idx].reshape(group, full_cap, width)
            recv_rows = lax.all_to_all(send_rows, "g", 0, 0, tiled=True)
            slots = lax.iota(jnp.int32, 2 * n)
            _, merge_order = lax.sort((windows.reshape(-1), slots), num_keys=1)
            rows = recv_rows.reshape(-1, width)[merge_order]
            return left - 1, jnp.where((slots < counts[0])[:, None], rows, 0.0)

        _, merged_rows = lax.while_loop(lambda carry: carry[0] > 0, padded, (need.reshape(()), merged_rows))
        return sorted_out.reshape(-1), merged_rows, counts

    row_spec = P(("batch", "g"))
    mat_spec = P(("batch", "g"), None)
    return jax.shard_map(local_part, mesh=mesh, in_specs=(row_spec, mat_spec), out_specs=(row_spec, mat_spec, row_spec), check_vma=False)
```

```python
import functools

import jax
import jax.numpy as jnp
from jax import lax
from jax.experimental import pallas as pl
from jax.experimental.pallas import tpu as pltpu
from jax.sharding import PartitionSpec as P

PAD_KEY = 128.0
LANES = 128
MESH = pl.DeviceIdType.MESH


def lane_prefix(x, lane):
    for step in (1, 2, 4):
        x = x + jnp.where(lane >= step, pltpu.roll(x, step, 1), 0)
    return x


def sub_prefix(x, sub):
    for step in (1, 2, 4):
        x = x + jnp.where(sub >= step, pltpu.roll(x, step, 0), 0)
    return x


def merge_runs(keys, locs, run_vregs):
    num = len(keys)
    sub = lax.broadcasted_iota(jnp.int32, keys[0].shape, 0)
    lane = lax.broadcasted_iota(jnp.int32, keys[0].shape, 1)
    size = 2 * run_vregs
    while size <= num:
        dist = size // 2
        while dist:
            for v in range(num):
                if v & dist:
                    continue
                a, b = (v, v + dist) if not v & size else (v + dist, v)
                swap = keys[b] < keys[a]
                keys[a], keys[b] = jnp.where(swap, keys[b], keys[a]), jnp.where(swap, keys[a], keys[b])
                locs[a], locs[b] = jnp.where(swap, locs[b], locs[a]), jnp.where(swap, locs[a], locs[b])
            dist //= 2
        for axis, index, extent, steps in ((0, sub, 8, (4, 2, 1)), (1, lane, LANES, (64, 32, 16, 8, 4, 2, 1))):
            for step in steps:
                bit = jnp.bitwise_and(index, step) != 0
                for v in range(num):
                    up = bit if not v & size else jnp.logical_not(bit)

                    def other(x):
                        return jnp.where(bit, pltpu.roll(x, step, axis), pltpu.roll(x, extent - step, axis))

                    peer_key, peer_loc = other(keys[v]), other(locs[v])
                    take = jnp.logical_xor(peer_key < keys[v], up)
                    keys[v] = jnp.where(take, peer_key, keys[v])
                    locs[v] = jnp.where(take, peer_loc, locs[v])
        size *= 2
    return keys, locs


def exchange_kernel(group, n, cap, relay, pieces, keys_ref, order_ref, rows_hbm,
                    out_ref, mkey_ref, mloc_ref, win_ref, start_ref, own_ref, need_ref,
                    rows_ref, keys_pad, sample, samples, outbox, inbox, rows3, near, far1, far2, got, tab_ref, idx1_ref, idx2_ref,
                    tab, order, idx1_sm, idx2_sm, edge_sm,
                    sample_sems, box_sems, near_sems, half_sems, far1_sems, far2_sems, local_sems, load_sems):
    run_rows = n // LANES
    win_rows = 2 * run_rows // group
    box_rows = win_rows + 8
    me = lax.axis_index("g")
    order_copy = pltpu.make_async_copy(order_ref, order.at[pl.ds(0, n)], local_sems.at[0])
    tail_copy = pltpu.make_async_copy(
        order_ref.at[pl.ds(0, order.shape[0] - n)], order.at[pl.ds(n, order.shape[0] - n)], local_sems.at[1])
    order_copy.start()
    tail_copy.start()
    barrier = pltpu.get_barrier_semaphore()
    for off in range(1, group):
        pl.semaphore_signal(barrier, inc=1, device_id={"g": lax.rem(me + off, group)}, device_id_type=MESH)

    piece = n // pieces
    loads = []
    for p in range(pieces):
        at = pl.ds(p * piece, piece)
        loads.append(pltpu.make_async_copy(rows_hbm.at[at], rows_ref.at[at], load_sems.at[p]))
        loads[p].start()
    stride = run_rows // group
    sample[...] = jnp.concatenate([keys_ref[pl.ds(m * stride, 1)] for m in range(group)], axis=0)
    samples[me] = jnp.concatenate([keys_ref[pl.ds(m * stride, 1)] for m in range(group)], axis=0)
    keys_pad[pl.ds(0, run_rows)] = keys_ref[...]
    tail = keys_pad.shape[0] - run_rows
    keys_pad[pl.ds(run_rows, tail)] = jnp.full((tail, LANES), PAD_KEY, jnp.float32)

    def relayout(t, c):
        at = pl.multiple_of(t * 64, 64)
        rows3[pl.ds(at, 64)] = rows_ref[pl.ds(at, 64)].reshape(64, 2, LANES)
        return c

    def ready(lo, hi):
        for p in range(lo, hi):
            loads[p].wait()
            lax.fori_loop(p * piece // 64, (p + 1) * piece // 64, relayout, 0)

    ready(0, pieces // 4)
    pl.semaphore_wait(barrier, group - 1)

    def send(src, dst, sems, off):
        copy = pltpu.make_async_remote_copy(
            src_ref=src, dst_ref=dst, send_sem=sems.at[0, off], recv_sem=sems.at[1, off],
            device_id={"g": lax.rem(me + off, group)}, device_id_type=MESH)
        copy.start()
        return copy

    offsets = [2, 6, 4, 3, 7, 5, 1, 0]
    copies = [send(sample, samples.at[me], sample_sems, off) for off in offsets[:-1]]
    ready(pieces // 4, pieces)
    for copy in copies:
        copy.wait()

    count = group * group
    col = jnp.broadcast_to(samples[...].reshape(count, LANES)[:, 0:1], (count, LANES))
    r_id = lax.broadcasted_iota(jnp.int32, (count, LANES), 0)
    l_id = lax.broadcasted_iota(jnp.int32, (count, LANES), 1)
    row = jnp.sum(jnp.where(r_id == l_id, col, 0.0), axis=0, keepdims=True)
    less = (jnp.broadcast_to(row, (count, LANES)) < col) & (l_id < count)
    rank = jnp.sum(jnp.where(less, 1.0, 0.0), axis=1, keepdims=True)
    want = (group * l_id + group // 2).astype(jnp.float32)
    splitters = jnp.sum(jnp.where(jnp.broadcast_to(rank, (count, LANES)) == want, col, 0.0), axis=0, keepdims=True)
    below = [jnp.zeros((1, LANES), jnp.int32)]
    for j in range(1, group):
        below.append(jnp.sum(jnp.where(keys_ref[...] < splitters[0, j], 1, 0), axis=0, keepdims=True))
    below = jnp.sum(jnp.concatenate(below, axis=0), axis=1, keepdims=True)
    edges = [jnp.clip(below[j, 0], 0, n) for j in range(group)] + [jnp.int32(n)]

    lane = lax.broadcasted_iota(jnp.int32, (group, LANES), 1)
    sub = lax.broadcasted_iota(jnp.int32, (group, LANES), 0)
    mine = jnp.zeros((8, LANES), jnp.int32)
    for j in range(group):
        edge_sm[j] = edges[j]
        start_ref[j] = edges[j]
        mine = jnp.where(lane == j, edges[j + 1] - edges[j], mine)
    edge_sm[group] = edges[group]
    mine = mine.astype(jnp.float32)
    order_copy.wait()
    tail_copy.wait()

    def gather(dst, base, size, pick):
        unroll = next(u for u in (43, 40, 32, 16) if size % u == 0)

        def step(t, c):
            for u in range(unroll):
                dst[base + t * unroll + u] = pick(t * unroll, u)
            return c
        lax.fori_loop(0, size // unroll, step, 0)

    waits, firsts = [], []

    def direct(off, low=0, high=cap, sems=near_sems):
        start = edge_sm[lax.rem(me + off, group)] + low

        def pick(at, u):
            return rows3[order[(start + at) + u]]

        size = high - low
        if off:
            gather(near.at[off], low, size, pick)
            waits.append(send(near.at[off, pl.ds(low, size)], out_ref.at[pl.ds(me * cap + low, size)], sems, off))
        else:
            gather(out_ref, me * cap + low, size, pick)

    early = cap // 86 * 43
    for off in offsets[:2]:
        direct(off, 0, early, half_sems)
    wl = lax.broadcasted_iota(jnp.int32, (win_rows, LANES), 1)
    pos = lax.broadcasted_iota(jnp.int32, (win_rows, LANES), 0) * LANES + wl
    for off in offsets:
        peer = lax.rem(me + off, group)
        start = edge_sm[peer]
        shift = jnp.bitwise_and(start, LANES - 1)
        at = jnp.clip(jnp.right_shift(start, LANES.bit_length() - 1), 0, run_rows)
        turn = jnp.bitwise_and(LANES - shift, LANES - 1)
        one = pltpu.roll(keys_pad[pl.ds(at, win_rows)], turn, 1)
        two = pltpu.roll(keys_pad[pl.ds(at + 1, win_rows)], turn, 1)
        window = jnp.where(pos < edge_sm[peer + 1] - start, jnp.where(wl < LANES - shift, one, two), PAD_KEY)
        if off:
            outbox[off, pl.ds(0, win_rows)] = window
            outbox[off, pl.ds(win_rows, 8)] = mine
        else:
            inbox[me, pl.ds(0, win_rows)] = window
            inbox[me, pl.ds(win_rows, 8)] = mine
    copies = [send(outbox.at[off], inbox.at[me], box_sems, off) for off in offsets[:-1]]
    for off in offsets[:2]:
        direct(off, early, cap)
    for copy in copies:
        copy.wait()
    counts = jnp.concatenate([inbox[s, pl.ds(win_rows, 1)] for s in range(group)], axis=0).astype(jnp.int32)
    counts = jnp.clip(counts, 0, n)
    over = jnp.maximum(counts - cap, 0)
    share = jnp.right_shift(over + (group - 1), group.bit_length() - 1)
    first = lane_prefix(share, lane) - share
    second = sub_prefix(share, sub) - share
    worst = jnp.maximum(jnp.max(first + share), jnp.max(second + share))
    for t, x in enumerate((counts, share, first, second)):
        tab_ref[t] = x
    to_smem = pltpu.make_async_copy(tab_ref, tab, local_sems.at[2])
    to_smem.start()
    direct(offsets[2])
    to_smem.wait()
    idx1 = jnp.zeros((group, LANES), jnp.int32)
    for j in range(group):
        q, a = tab[1, me, j], tab[2, me, j]
        src = edge_sm[j] + cap - a + q * sub + lane
        idx1 = jnp.where((lane >= a) & (lane < a + q), src, idx1)
    idx1_ref[...] = jnp.clip(idx1, 0, n - 1)
    idx1_copy = pltpu.make_async_copy(idx1_ref, idx1_sm, local_sems.at[3])
    idx1_copy.start()
    idx1_copy.wait()
    for off in offsets:
        peer = lax.rem(me + off, group)

        def pick(at, u):
            return rows3[order[idx1_sm[peer, at + u]]]

        if off:
            gather(far1.at[off], 0, relay, pick)
            firsts.append(send(far1.at[off], got.at[pl.ds(me * relay, relay)], far1_sems, off))
        else:
            gather(got, me * relay, relay, pick)
    for off in offsets[3:]:
        direct(off)

    lane1 = lane[0:1]
    for j in range(group):
        line = jnp.zeros((1, LANES), jnp.int32)
        for s in range(group):
            q, a, b = tab[1, s, j], tab[2, s, j], tab[3, s, j]
            line = jnp.where((lane1 >= b) & (lane1 < b + q), s * relay + a - b + lane1, line)
        idx2_ref[pl.ds(j, 1)] = jnp.clip(line, 0, group * relay - 1)
    idx2_copy = pltpu.make_async_copy(idx2_ref, idx2_sm, local_sems.at[4])
    idx2_copy.start()

    own = jnp.int32(0)
    run_keys, run_locs = [], []
    for s in range(group):
        num, q, b = tab[0, s, me], tab[1, s, me], tab[3, s, me]
        own = own + num
        window = inbox[s, pl.ds(0, win_rows)]
        win_ref[pl.ds(s * win_rows, win_rows)] = window
        where = pos
        if s % 2:
            window = jnp.take_along_axis(window, LANES - 1 - wl, axis=1)
            window = jnp.concatenate([window[r:r + 1] for r in range(win_rows - 1, -1, -1)], axis=0)
            where = win_rows * LANES - 1 - pos
        extra = where - cap
        far = group * cap + b + extra
        for m in range(1, group):
            far = far + jnp.where(extra >= m * q, relay - q, 0)
        loc = jnp.where(where < cap, s * cap + where, far)
        loc = jnp.where(where < num, jnp.clip(loc, 0, group * (cap + relay) - 1), 0)
        for v in range(win_rows // 8):
            run_keys.append(window[v * 8:v * 8 + 8])
            run_locs.append(loc[v * 8:v * 8 + 8])
    own_ref[0] = own
    need_ref[0] = jnp.where(worst <= relay, 0, 1)
    merged, placed = merge_runs(run_keys, run_locs, win_rows // 8)
    for v in range(2 * run_rows // 8):
        mkey_ref[pl.ds(v * 8, 8)] = merged[v]
        mloc_ref[pl.ds(v * 8, 8)] = placed[v]

    idx2_copy.wait()
    for copy in firsts:
        copy.wait()
    base2 = group * cap + me * relay
    for off in offsets:
        peer = lax.rem(me + off, group)

        def pick(at, u):
            return got[idx2_sm[peer, at + u]]

        if off:
            gather(far2.at[off], 0, relay, pick)
            waits.append(send(far2.at[off], out_ref.at[pl.ds(base2, relay)], far2_sems, off))
        else:
            gather(out_ref, base2, relay, pick)
    for copy in waits:
        copy.wait()


def place_kernel(block, chunk, loc_ref, own_ref, rows_ref, keys_ref, out_ref, out_own_ref, out_keys_ref,
                 loc, bufs, blanks, tmp_a, tmp_b, loc_sems, out_sems, blank_sems, key_sem):
    blocks = out_ref.shape[0] // block
    width = out_ref.shape[1]
    own = jnp.clip(own_ref[0], 0, out_ref.shape[0])
    out_own_ref[0] = own
    used = (own + block - 1) // block

    def loc_copy(b):
        at = pl.ds(pl.multiple_of(b * block, block), block)
        return pltpu.make_async_copy(loc_ref.at[at], loc.at[at], loc_sems.at[b])

    def out_copy(b, src, sem):
        return pltpu.make_async_copy(src, out_ref.at[pl.ds(pl.multiple_of(b * block, block), block)], sem)

    for b in range(blocks):
        loc_copy(b).start()
    keys_copy = pltpu.make_async_copy(keys_ref, out_keys_ref, key_sem)
    keys_copy.start()
    blanks[...] = jnp.zeros_like(blanks)

    def blank(b, c):
        out_copy(b, blanks, blank_sems.at[b]).start()
        return c

    lax.fori_loop(used, blocks, blank, 0)

    def fetch(base, tmp):
        for u in range(chunk):
            tmp[u] = rows_ref[loc[base + u]]

    def one_block(b, carry):
        slot = lax.rem(b, 2)
        base = b * block
        num = jnp.minimum(own - base, block)
        loc_copy(b).wait()

        @pl.when(b >= 2)
        def _():
            out_copy(b - 2, bufs.at[slot], out_sems.at[slot]).wait()

        def finish(c, tmp):
            bufs[slot, pl.ds(pl.multiple_of(c * chunk, chunk), chunk)] = tmp[...].reshape(chunk, width)

        fetch(base, tmp_a)

        def step(t, c):
            fetch(base + (2 * t + 1) * chunk, tmp_b)
            finish(2 * t, tmp_a)
            fetch(base + jnp.minimum(2 * t + 2, block // chunk - 1) * chunk, tmp_a)
            finish(2 * t + 1, tmp_b)
            return c

        lax.fori_loop(0, (num + 2 * chunk - 1) // (2 * chunk), step, 0)

        @pl.when(num < block)
        def _():
            edge = num // chunk
            at = pl.multiple_of(edge * chunk, chunk)
            row = at + lax.broadcasted_iota(jnp.int32, (chunk, width), 0)
            x = bufs[slot, pl.ds(at, chunk)]
            bufs[slot, pl.ds(at, chunk)] = jnp.where(row < num, x, jnp.zeros_like(x))

            def clear(t, c):
                bufs[slot, pl.ds(pl.multiple_of(t * chunk, chunk), chunk)] = jnp.zeros((chunk, width), bufs.dtype)
                return c

            lax.fori_loop(edge + 1, block // chunk, clear, 0)

        out_copy(b, bufs.at[slot], out_sems.at[slot]).start()
        return carry

    lax.fori_loop(0, used, one_block, 0)
    for back in (2, 1):
        @pl.when(used >= back)
        def _():
            b = used - back
            slot = lax.rem(b, 2)
            out_copy(b, bufs.at[slot], out_sems.at[slot]).wait()

    keys_copy.wait()

    def settle(b, c):
        out_copy(b, blanks, blank_sems.at[b]).wait()
        return c

    lax.fori_loop(used, blocks, settle, 0)

    def skip(b, c):
        loc_copy(b).wait()
        return c

    lax.fori_loop(used, blocks, skip, 0)


def solution(mesh):
    group = mesh.shape["g"]

    def local_part(keys_loc, rows_loc):
        n = keys_loc.shape[0]
        width = rows_loc.shape[1]
        full_cap = 2 * n // group
        cap = n // group + n // group // 128
        relay = LANES
        total = group * (cap + relay)
        spec = lambda m: pl.BlockSpec(memory_space=m)
        vmem, smem = pltpu.VMEM, pltpu.SMEM
        dtype = rows_loc.dtype
        run_rows = n // LANES
        pad = -(-cap // LANES) * LANES

        sorted_keys, order = lax.sort((keys_loc, lax.iota(jnp.int32, n)), num_keys=1)
        recv, merged_keys, merged_loc, windows, my_starts, own, need = pl.pallas_call(
            functools.partial(exchange_kernel, group, n, cap, relay, 8),
            out_shape=[
                jax.ShapeDtypeStruct((total, 2, LANES), dtype),
                jax.ShapeDtypeStruct((2 * run_rows, LANES), jnp.float32),
                jax.ShapeDtypeStruct((2 * run_rows, LANES), jnp.int32),
                jax.ShapeDtypeStruct((2 * run_rows, LANES), jnp.float32),
                jax.ShapeDtypeStruct((group,), jnp.int32),
                jax.ShapeDtypeStruct((1,), jnp.int32),
                jax.ShapeDtypeStruct((1,), jnp.int32),
            ],
            in_specs=[spec(vmem), spec(pl.ANY), spec(pl.ANY)],
            out_specs=[spec(vmem)] * 4 + [spec(smem)] * 3,
            scratch_shapes=[
                pltpu.VMEM((n, width), dtype),
                pltpu.VMEM((run_rows + 24, LANES), jnp.float32),
                pltpu.VMEM((group, LANES), jnp.float32),
                pltpu.VMEM((group, group, LANES), jnp.float32),
                pltpu.VMEM((group, 2 * run_rows // group + 8, LANES), jnp.float32),
                pltpu.VMEM((group, 2 * run_rows // group + 8, LANES), jnp.float32),
                pltpu.VMEM((n, 2, LANES), dtype),
                pltpu.VMEM((group, cap, 2, LANES), dtype),
                pltpu.VMEM((group, relay, 2, LANES), dtype),
                pltpu.VMEM((group, relay, 2, LANES), dtype),
                pltpu.VMEM((group * relay, 2, LANES), dtype),
                pltpu.VMEM((4, group, LANES), jnp.int32),
                pltpu.VMEM((group, LANES), jnp.int32),
                pltpu.VMEM((group, LANES), jnp.int32),
                pltpu.SMEM((4, group, LANES), jnp.int32),
                pltpu.SMEM((n + pad,), jnp.int32),
                pltpu.SMEM((group, LANES), jnp.int32),
                pltpu.SMEM((group, LANES), jnp.int32),
                pltpu.SMEM((group + 1,), jnp.int32),
            ] + [pltpu.SemaphoreType.DMA((2, group))] * 6 + [pltpu.SemaphoreType.DMA((5,)), pltpu.SemaphoreType.DMA((8,))],
            compiler_params=pltpu.CompilerParams(collective_id=0, has_side_effects=True, vmem_limit_bytes=32 << 20),
            name="exchange",
        )(sorted_keys.reshape(run_rows, LANES), order, rows_loc)

        block = 1024
        chunk = 64
        blocks = 2 * n // block
        merged_rows, counts, sorted_out = pl.pallas_call(
            functools.partial(place_kernel, block, chunk),
            out_shape=[
                jax.ShapeDtypeStruct((2 * n, width), dtype),
                jax.ShapeDtypeStruct((1,), jnp.int32),
                jax.ShapeDtypeStruct((2 * run_rows, LANES), jnp.float32),
            ],
            in_specs=[spec(pl.ANY), spec(smem), spec(vmem), spec(vmem)],
            out_specs=[spec(pl.ANY), spec(smem), spec(pl.ANY)],
            scratch_shapes=[
                pltpu.SMEM((2 * n,), jnp.int32),
                pltpu.VMEM((2, block, width), dtype),
                pltpu.VMEM((block, width), dtype),
                pltpu.VMEM((chunk, 2, LANES), dtype),
                pltpu.VMEM((chunk, 2, LANES), dtype),
                pltpu.SemaphoreType.DMA((blocks,)),
                pltpu.SemaphoreType.DMA((2,)),
                pltpu.SemaphoreType.DMA((blocks,)),
                pltpu.SemaphoreType.DMA,
            ],
            compiler_params=pltpu.CompilerParams(vmem_limit_bytes=16 << 20),
            name="place",
        )(merged_loc.reshape(-1), own, recv, merged_keys)

        merged_rows, windows, my_starts, need = lax.optimization_barrier((merged_rows, windows, my_starts, need))

        def padded(carry):
            left, _ = carry
            order_pad = jnp.concatenate([order, jnp.zeros((full_cap,), jnp.int32)])
            at = my_starts + (left - 1)
            send_idx = jnp.concatenate([lax.dynamic_slice(order_pad, (at[d],), (full_cap,)) for d in range(group)])
            send_rows = rows_loc[send_idx].reshape(group, full_cap, width)
            recv_rows = lax.all_to_all(send_rows, "g", 0, 0, tiled=True)
            slots = lax.iota(jnp.int32, 2 * n)
            _, merge_order = lax.sort((windows.reshape(-1), slots), num_keys=1)
            rows = recv_rows.reshape(-1, width)[merge_order]
            return left - 1, jnp.where((slots < counts[0])[:, None], rows, 0.0)

        _, merged_rows = lax.while_loop(lambda carry: carry[0] > 0, padded, (need.reshape(()), merged_rows))
        return sorted_out.reshape(-1), merged_rows, counts

    row_spec = P(("batch", "g"))
    mat_spec = P(("batch", "g"), None)
    return jax.shard_map(local_part, mesh=mesh, in_specs=(row_spec, mat_spec), out_specs=(row_spec, mat_spec, row_spec), check_vma=False)
```

```python
import functools

import jax
import jax.numpy as jnp
from jax import lax
from jax.experimental import pallas as pl
from jax.experimental.pallas import tpu as pltpu
from jax.sharding import PartitionSpec as P

PAD_KEY = 128.0
LANES = 128
MESH = pl.DeviceIdType.MESH


def lane_prefix(x, lane):
    for step in (1, 2, 4):
        x = x + jnp.where(lane >= step, pltpu.roll(x, step, 1), 0)
    return x


def sub_prefix(x, sub):
    for step in (1, 2, 4):
        x = x + jnp.where(sub >= step, pltpu.roll(x, step, 0), 0)
    return x


def merge_runs(keys, locs, run_vregs):
    num = len(keys)
    sub = lax.broadcasted_iota(jnp.int32, keys[0].shape, 0)
    lane = lax.broadcasted_iota(jnp.int32, keys[0].shape, 1)
    size = 2 * run_vregs
    while size <= num:
        dist = size // 2
        while dist:
            for v in range(num):
                if v & dist:
                    continue
                a, b = (v, v + dist) if not v & size else (v + dist, v)
                swap = keys[b] < keys[a]
                keys[a], keys[b] = jnp.where(swap, keys[b], keys[a]), jnp.where(swap, keys[a], keys[b])
                locs[a], locs[b] = jnp.where(swap, locs[b], locs[a]), jnp.where(swap, locs[a], locs[b])
            dist //= 2
        for axis, index, extent, steps in ((0, sub, 8, (4, 2, 1)), (1, lane, LANES, (64, 32, 16, 8, 4, 2, 1))):
            for step in steps:
                bit = jnp.bitwise_and(index, step) != 0
                for v in range(num):
                    up = bit if not v & size else jnp.logical_not(bit)

                    def other(x):
                        return jnp.where(bit, pltpu.roll(x, step, axis), pltpu.roll(x, extent - step, axis))

                    peer_key, peer_loc = other(keys[v]), other(locs[v])
                    take = jnp.logical_xor(peer_key < keys[v], up)
                    keys[v] = jnp.where(take, peer_key, keys[v])
                    locs[v] = jnp.where(take, peer_loc, locs[v])
        size *= 2
    return keys, locs


def exchange_kernel(group, n, cap, relay, pieces, keys_ref, order_ref, rows_hbm,
                    out_ref, mkey_ref, mloc_ref, win_ref, start_ref, own_ref, need_ref,
                    rows_ref, keys_pad, sample, samples, outbox, inbox, rows3, near, far1, far2, got, tab_ref, idx1_ref, idx2_ref,
                    tab, order, idx1_sm, idx2_sm, edge_sm,
                    sample_sems, box_sems, near_sems, half_sems, far1_sems, far2_sems, local_sems, load_sems):
    run_rows = n // LANES
    win_rows = 2 * run_rows // group
    box_rows = win_rows + 8
    me = lax.axis_index("g")
    order_copy = pltpu.make_async_copy(order_ref, order.at[pl.ds(0, n)], local_sems.at[0])
    tail_copy = pltpu.make_async_copy(
        order_ref.at[pl.ds(0, order.shape[0] - n)], order.at[pl.ds(n, order.shape[0] - n)], local_sems.at[1])
    order_copy.start()
    tail_copy.start()
    barrier = pltpu.get_barrier_semaphore()
    for off in range(1, group):
        pl.semaphore_signal(barrier, inc=1, device_id={"g": lax.rem(me + off, group)}, device_id_type=MESH)

    piece = n // pieces
    loads = []
    for p in range(pieces):
        at = pl.ds(p * piece, piece)
        loads.append(pltpu.make_async_copy(rows_hbm.at[at], rows_ref.at[at], load_sems.at[p]))
        loads[p].start()
    stride = run_rows // group
    sample[...] = jnp.concatenate([keys_ref[pl.ds(m * stride, 1)] for m in range(group)], axis=0)
    samples[me] = jnp.concatenate([keys_ref[pl.ds(m * stride, 1)] for m in range(group)], axis=0)
    keys_pad[pl.ds(0, run_rows)] = keys_ref[...]
    tail = keys_pad.shape[0] - run_rows
    keys_pad[pl.ds(run_rows, tail)] = jnp.full((tail, LANES), PAD_KEY, jnp.float32)

    def relayout(t, c):
        at = pl.multiple_of(t * 64, 64)
        rows3[pl.ds(at, 64)] = rows_ref[pl.ds(at, 64)].reshape(64, 2, LANES)
        return c

    def ready(lo, hi):
        for p in range(lo, hi):
            loads[p].wait()
            lax.fori_loop(p * piece // 64, (p + 1) * piece // 64, relayout, 0)

    ready(0, pieces // 4)
    pl.semaphore_wait(barrier, group - 1)

    def send(src, dst, sems, off):
        copy = pltpu.make_async_remote_copy(
            src_ref=src, dst_ref=dst, send_sem=sems.at[0, off], recv_sem=sems.at[1, off],
            device_id={"g": lax.rem(me + off, group)}, device_id_type=MESH)
        copy.start()
        return copy

    offsets = [2, 6, 4, 3, 7, 5, 1, 0]
    copies = [send(sample, samples.at[me], sample_sems, off) for off in offsets[:-1]]
    ready(pieces // 4, pieces)
    for copy in copies:
        copy.wait()

    count = group * group
    col = jnp.broadcast_to(samples[...].reshape(count, LANES)[:, 0:1], (count, LANES))
    r_id = lax.broadcasted_iota(jnp.int32, (count, LANES), 0)
    l_id = lax.broadcasted_iota(jnp.int32, (count, LANES), 1)
    row = jnp.sum(jnp.where(r_id == l_id, col, 0.0), axis=0, keepdims=True)
    less = (jnp.broadcast_to(row, (count, LANES)) < col) & (l_id < count)
    rank = jnp.sum(jnp.where(less, 1.0, 0.0), axis=1, keepdims=True)
    want = (group * l_id + group // 2).astype(jnp.float32)
    splitters = jnp.sum(jnp.where(jnp.broadcast_to(rank, (count, LANES)) == want, col, 0.0), axis=0, keepdims=True)
    below = [jnp.zeros((1, LANES), jnp.int32)]
    for j in range(1, group):
        below.append(jnp.sum(jnp.where(keys_ref[...] < splitters[0, j], 1, 0), axis=0, keepdims=True))
    below = jnp.sum(jnp.concatenate(below, axis=0), axis=1, keepdims=True)
    edges = [jnp.clip(below[j, 0], 0, n) for j in range(group)] + [jnp.int32(n)]

    lane = lax.broadcasted_iota(jnp.int32, (group, LANES), 1)
    sub = lax.broadcasted_iota(jnp.int32, (group, LANES), 0)
    mine = jnp.zeros((8, LANES), jnp.int32)
    for j in range(group):
        edge_sm[j] = edges[j]
        start_ref[j] = edges[j]
        mine = jnp.where(lane == j, edges[j + 1] - edges[j], mine)
    edge_sm[group] = edges[group]
    mine = mine.astype(jnp.float32)
    order_copy.wait()
    tail_copy.wait()

    def gather(dst, base, size, pick):
        unroll = next(u for u in (43, 40, 32, 16) if size % u == 0)

        def step(t, c):
            for u in range(unroll):
                dst[base + t * unroll + u] = pick(t * unroll, u)
            return c
        lax.fori_loop(0, size // unroll, step, 0)

    waits, firsts = [], []

    def direct(off, low=0, high=cap, sems=near_sems):
        start = edge_sm[lax.rem(me + off, group)] + low

        def pick(at, u):
            return rows3[order[(start + at) + u]]

        size = high - low
        if off:
            gather(near.at[off], low, size, pick)
            waits.append(send(near.at[off, pl.ds(low, size)], out_ref.at[pl.ds(me * cap + low, size)], sems, off))
        else:
            gather(out_ref, me * cap + low, size, pick)

    early = cap // 86 * 43
    for off in offsets[:2]:
        direct(off, 0, early, half_sems)
    wl = lax.broadcasted_iota(jnp.int32, (win_rows, LANES), 1)
    pos = lax.broadcasted_iota(jnp.int32, (win_rows, LANES), 0) * LANES + wl
    for off in offsets:
        peer = lax.rem(me + off, group)
        start = edge_sm[peer]
        shift = jnp.bitwise_and(start, LANES - 1)
        at = jnp.clip(jnp.right_shift(start, LANES.bit_length() - 1), 0, run_rows)
        turn = jnp.bitwise_and(LANES - shift, LANES - 1)
        one = pltpu.roll(keys_pad[pl.ds(at, win_rows)], turn, 1)
        two = pltpu.roll(keys_pad[pl.ds(at + 1, win_rows)], turn, 1)
        window = jnp.where(pos < edge_sm[peer + 1] - start, jnp.where(wl < LANES - shift, one, two), PAD_KEY)
        if off:
            outbox[off, pl.ds(0, win_rows)] = window
            outbox[off, pl.ds(win_rows, 8)] = mine
        else:
            inbox[me, pl.ds(0, win_rows)] = window
            inbox[me, pl.ds(win_rows, 8)] = mine
    copies = [send(outbox.at[off], inbox.at[me], box_sems, off) for off in offsets[:-1]]
    for off in offsets[:2]:
        direct(off, early, cap)
    for copy in copies:
        copy.wait()
    counts = jnp.concatenate([inbox[s, pl.ds(win_rows, 1)] for s in range(group)], axis=0).astype(jnp.int32)
    counts = jnp.clip(counts, 0, n)
    over = jnp.maximum(counts - cap, 0)
    share = jnp.right_shift(over + (group - 1), group.bit_length() - 1)
    first = lane_prefix(share, lane) - share
    second = sub_prefix(share, sub) - share
    worst = jnp.maximum(jnp.max(first + share), jnp.max(second + share))
    for t, x in enumerate((counts, share, first, second)):
        tab_ref[t] = x
    to_smem = pltpu.make_async_copy(tab_ref, tab, local_sems.at[2])
    to_smem.start()
    direct(offsets[2])
    to_smem.wait()
    idx1 = jnp.zeros((group, LANES), jnp.int32)
    for j in range(group):
        q, a = tab[1, me, j], tab[2, me, j]
        src = edge_sm[j] + cap - a + q * sub + lane
        idx1 = jnp.where((lane >= a) & (lane < a + q), src, idx1)
    idx1_ref[...] = jnp.clip(idx1, 0, n - 1)
    idx1_copy = pltpu.make_async_copy(idx1_ref, idx1_sm, local_sems.at[3])
    idx1_copy.start()
    idx1_copy.wait()
    for off in offsets:
        peer = lax.rem(me + off, group)

        def pick(at, u):
            return rows3[order[idx1_sm[peer, at + u]]]

        if off:
            gather(far1.at[off], 0, relay, pick)
            firsts.append(send(far1.at[off], got.at[pl.ds(me * relay, relay)], far1_sems, off))
        else:
            gather(got, me * relay, relay, pick)
    for off in offsets[3:]:
        direct(off)

    lane1 = lane[0:1]
    for j in range(group):
        line = jnp.zeros((1, LANES), jnp.int32)
        for s in range(group):
            q, a, b = tab[1, s, j], tab[2, s, j], tab[3, s, j]
            line = jnp.where((lane1 >= b) & (lane1 < b + q), s * relay + a - b + lane1, line)
        idx2_ref[pl.ds(j, 1)] = jnp.clip(line, 0, group * relay - 1)
    idx2_copy = pltpu.make_async_copy(idx2_ref, idx2_sm, local_sems.at[4])
    idx2_copy.start()

    own = jnp.int32(0)
    run_keys, run_locs = [], []
    for s in range(group):
        num, q, b = tab[0, s, me], tab[1, s, me], tab[3, s, me]
        own = own + num
        window = inbox[s, pl.ds(0, win_rows)]
        win_ref[pl.ds(s * win_rows, win_rows)] = window
        where = pos
        if s % 2:
            window = jnp.take_along_axis(window, LANES - 1 - wl, axis=1)
            window = jnp.concatenate([window[r:r + 1] for r in range(win_rows - 1, -1, -1)], axis=0)
            where = win_rows * LANES - 1 - pos
        extra = where - cap
        far = group * cap + b + extra
        for m in range(1, group):
            far = far + jnp.where(extra >= m * q, relay - q, 0)
        loc = jnp.where(where < cap, s * cap + where, far)
        loc = jnp.where(where < num, jnp.clip(loc, 0, group * (cap + relay) - 1), 0)
        for v in range(win_rows // 8):
            run_keys.append(window[v * 8:v * 8 + 8])
            run_locs.append(loc[v * 8:v * 8 + 8])
    own_ref[0] = own
    need_ref[0] = jnp.where(worst <= relay, 0, 1)
    merged, placed = merge_runs(run_keys, run_locs, win_rows // 8)
    for v in range(2 * run_rows // 8):
        mkey_ref[pl.ds(v * 8, 8)] = merged[v]
        mloc_ref[pl.ds(v * 8, 8)] = placed[v]

    idx2_copy.wait()
    for copy in firsts:
        copy.wait()
    base2 = group * cap + me * relay
    for off in offsets:
        peer = lax.rem(me + off, group)

        def pick(at, u):
            return got[idx2_sm[peer, at + u]]

        if off:
            gather(far2.at[off], 0, relay, pick)
            waits.append(send(far2.at[off], out_ref.at[pl.ds(base2, relay)], far2_sems, off))
        else:
            gather(out_ref, base2, relay, pick)
    for copy in waits:
        copy.wait()


def place_kernel(block, chunk, loc_ref, own_ref, rows_ref, keys_ref, out_ref, out_own_ref, out_keys_ref,
                 loc, bufs, blanks, tmp_a, tmp_b, loc_sems, out_sems, blank_sems, key_sem):
    blocks = out_ref.shape[0] // block
    width = out_ref.shape[1]
    own = jnp.clip(own_ref[0], 0, out_ref.shape[0])
    out_own_ref[0] = own
    used = (own + block - 1) // block

    def loc_copy(b):
        at = pl.ds(pl.multiple_of(b * block, block), block)
        return pltpu.make_async_copy(loc_ref.at[at], loc.at[at], loc_sems.at[b])

    def out_copy(b, src, sem):
        return pltpu.make_async_copy(src, out_ref.at[pl.ds(pl.multiple_of(b * block, block), block)], sem)

    for b in range(blocks):
        loc_copy(b).start()
    keys_copy = pltpu.make_async_copy(keys_ref, out_keys_ref, key_sem)
    keys_copy.start()
    blanks[...] = jnp.zeros_like(blanks)

    def blank(b, c):
        out_copy(b, blanks, blank_sems.at[b]).start()
        return c

    lax.fori_loop(used, blocks, blank, 0)

    def fetch(base, tmp):
        for u in range(chunk):
            tmp[u] = rows_ref[loc[base + u]]

    def one_block(b, carry):
        slot = lax.rem(b, 2)
        base = b * block
        num = jnp.minimum(own - base, block)
        loc_copy(b).wait()

        @pl.when(b >= 2)
        def _():
            out_copy(b - 2, bufs.at[slot], out_sems.at[slot]).wait()

        def finish(c, tmp):
            bufs[slot, pl.ds(pl.multiple_of(c * chunk, chunk), chunk)] = tmp[...].reshape(chunk, width)

        fetch(base, tmp_a)

        def step(t, c):
            fetch(base + (2 * t + 1) * chunk, tmp_b)
            finish(2 * t, tmp_a)
            fetch(base + jnp.minimum(2 * t + 2, block // chunk - 1) * chunk, tmp_a)
            finish(2 * t + 1, tmp_b)
            return c

        lax.fori_loop(0, (num + 2 * chunk - 1) // (2 * chunk), step, 0)

        @pl.when(num < block)
        def _():
            edge = num // chunk
            at = pl.multiple_of(edge * chunk, chunk)
            row = at + lax.broadcasted_iota(jnp.int32, (chunk, width), 0)
            x = bufs[slot, pl.ds(at, chunk)]
            bufs[slot, pl.ds(at, chunk)] = jnp.where(row < num, x, jnp.zeros_like(x))

            def clear(t, c):
                bufs[slot, pl.ds(pl.multiple_of(t * chunk, chunk), chunk)] = jnp.zeros((chunk, width), bufs.dtype)
                return c

            lax.fori_loop(edge + 1, block // chunk, clear, 0)

        out_copy(b, bufs.at[slot], out_sems.at[slot]).start()
        return carry

    lax.fori_loop(0, used, one_block, 0)
    for back in (2, 1):
        @pl.when(used >= back)
        def _():
            b = used - back
            slot = lax.rem(b, 2)
            out_copy(b, bufs.at[slot], out_sems.at[slot]).wait()

    keys_copy.wait()

    def settle(b, c):
        out_copy(b, blanks, blank_sems.at[b]).wait()
        return c

    lax.fori_loop(used, blocks, settle, 0)

    def skip(b, c):
        loc_copy(b).wait()
        return c

    lax.fori_loop(used, blocks, skip, 0)


def solution(mesh):
    group = mesh.shape["g"]

    def local_part(keys_loc, rows_loc):
        n = keys_loc.shape[0]
        width = rows_loc.shape[1]
        full_cap = 2 * n // group
        cap = n // group + n // group // 128
        relay = LANES
        total = group * (cap + relay)
        spec = lambda m: pl.BlockSpec(memory_space=m)
        vmem, smem = pltpu.VMEM, pltpu.SMEM
        dtype = rows_loc.dtype
        run_rows = n // LANES
        pad = -(-cap // LANES) * LANES

        sorted_keys, order = lax.sort((keys_loc, lax.iota(jnp.int32, n)), num_keys=1)
        recv, merged_keys, merged_loc, windows, my_starts, own, need = pl.pallas_call(
            functools.partial(exchange_kernel, group, n, cap, relay, 8),
            out_shape=[
                jax.ShapeDtypeStruct((total, 2, LANES), dtype),
                jax.ShapeDtypeStruct((2 * run_rows, LANES), jnp.float32),
                jax.ShapeDtypeStruct((2 * run_rows, LANES), jnp.int32),
                jax.ShapeDtypeStruct((2 * run_rows, LANES), jnp.float32),
                jax.ShapeDtypeStruct((group,), jnp.int32),
                jax.ShapeDtypeStruct((1,), jnp.int32),
                jax.ShapeDtypeStruct((1,), jnp.int32),
            ],
            in_specs=[spec(vmem), spec(pl.ANY), spec(pl.ANY)],
            out_specs=[spec(vmem)] * 4 + [spec(smem)] * 3,
            scratch_shapes=[
                pltpu.VMEM((n, width), dtype),
                pltpu.VMEM((run_rows + 24, LANES), jnp.float32),
                pltpu.VMEM((group, LANES), jnp.float32),
                pltpu.VMEM((group, group, LANES), jnp.float32),
                pltpu.VMEM((group, 2 * run_rows // group + 8, LANES), jnp.float32),
                pltpu.VMEM((group, 2 * run_rows // group + 8, LANES), jnp.float32),
                pltpu.VMEM((n, 2, LANES), dtype),
                pltpu.VMEM((group, cap, 2, LANES), dtype),
                pltpu.VMEM((group, relay, 2, LANES), dtype),
                pltpu.VMEM((group, relay, 2, LANES), dtype),
                pltpu.VMEM((group * relay, 2, LANES), dtype),
                pltpu.VMEM((4, group, LANES), jnp.int32),
                pltpu.VMEM((group, LANES), jnp.int32),
                pltpu.VMEM((group, LANES), jnp.int32),
                pltpu.SMEM((4, group, LANES), jnp.int32),
                pltpu.SMEM((n + pad,), jnp.int32),
                pltpu.SMEM((group, LANES), jnp.int32),
                pltpu.SMEM((group, LANES), jnp.int32),
                pltpu.SMEM((group + 1,), jnp.int32),
            ] + [pltpu.SemaphoreType.DMA((2, group))] * 6 + [pltpu.SemaphoreType.DMA((5,)), pltpu.SemaphoreType.DMA((8,))],
            compiler_params=pltpu.CompilerParams(collective_id=0, has_side_effects=True, vmem_limit_bytes=32 << 20),
            name="exchange",
        )(sorted_keys.reshape(run_rows, LANES), order, rows_loc)

        block = 2048
        chunk = 64
        blocks = 2 * n // block
        merged_rows, counts, sorted_out = pl.pallas_call(
            functools.partial(place_kernel, block, chunk),
            out_shape=[
                jax.ShapeDtypeStruct((2 * n, width), dtype),
                jax.ShapeDtypeStruct((1,), jnp.int32),
                jax.ShapeDtypeStruct((2 * run_rows, LANES), jnp.float32),
            ],
            in_specs=[spec(pl.ANY), spec(smem), spec(vmem), spec(vmem)],
            out_specs=[spec(pl.ANY), spec(smem), spec(pl.ANY)],
            scratch_shapes=[
                pltpu.SMEM((2 * n,), jnp.int32),
                pltpu.VMEM((2, block, width), dtype),
                pltpu.VMEM((block, width), dtype),
                pltpu.VMEM((chunk, 2, LANES), dtype),
                pltpu.VMEM((chunk, 2, LANES), dtype),
                pltpu.SemaphoreType.DMA((blocks,)),
                pltpu.SemaphoreType.DMA((2,)),
                pltpu.SemaphoreType.DMA((blocks,)),
                pltpu.SemaphoreType.DMA,
            ],
            compiler_params=pltpu.CompilerParams(vmem_limit_bytes=16 << 20),
            name="place",
        )(merged_loc.reshape(-1), own, recv, merged_keys)

        merged_rows, windows, my_starts, need = lax.optimization_barrier((merged_rows, windows, my_starts, need))

        def padded(carry):
            left, _ = carry
            order_pad = jnp.concatenate([order, jnp.zeros((full_cap,), jnp.int32)])
            at = my_starts + (left - 1)
            send_idx = jnp.concatenate([lax.dynamic_slice(order_pad, (at[d],), (full_cap,)) for d in range(group)])
            send_rows = rows_loc[send_idx].reshape(group, full_cap, width)
            recv_rows = lax.all_to_all(send_rows, "g", 0, 0, tiled=True)
            slots = lax.iota(jnp.int32, 2 * n)
            _, merge_order = lax.sort((windows.reshape(-1), slots), num_keys=1)
            rows = recv_rows.reshape(-1, width)[merge_order]
            return left - 1, jnp.where((slots < counts[0])[:, None], rows, 0.0)

        _, merged_rows = lax.while_loop(lambda carry: carry[0] > 0, padded, (need.reshape(()), merged_rows))
        return sorted_out.reshape(-1), merged_rows, counts

    row_spec = P(("batch", "g"))
    mat_spec = P(("batch", "g"), None)
    return jax.shard_map(local_part, mesh=mesh, in_specs=(row_spec, mat_spec), out_specs=(row_spec, mat_spec, row_spec), check_vma=False)
```
